32 devices in a mesh: rep: 2 (over x), mp: 16 (over z, y, core).
Axes of the slice: x: 2, y: 2, z: 4, core: 2. Of those that a mesh axis runs over, the one named last changes fastest.
Arguments:
- tokens: bfloat16 [1280, 3072], P(('rep', 'mp')), may hold values from -6 to 6
- w_in: bfloat16 [2, 3072, 2, 12288], P('rep', None, None, 'mp'), may hold values from -0.109375 to 0.109375
- w_down: bfloat16 [2, 12288, 3072], P('rep', 'mp'), may hold values from -0.0546875 to 0.0546875
- norm_gain: float32 [3072], replicated, may hold values from 0.1 to 1.9
- final_gain: float32 [3072], replicated, may hold values from 0.1 to 1.9
- value_head: float32 [3072], replicated, may hold values from -0.6 to 0.6
- owner: int32 [16], P('mp'), may hold values from 0 to 1
- lengths: int32 [16], P('rep'), may hold values from 20 to 80, as said below
- offsets: int32 [16], P('rep'), may hold values from 0 to 620, as said below
Outputs:
- mixed: bfloat16 [1280, 3072], P(('rep', 'mp'))
- rewards: float32 [16], P('rep')
The draws below stay inside these ranges and needn't reach their ends.
Inputs may be any that keep to these rules, and one draw needn't show every extreme that they name: `lengths`: every rollout is at least a quarter of 80 long; in each group one rollout has exactly 80 tokens. `offsets`: rollout j of a group lies wholly within slots j * 80 to (j + 1) * 80 - 1 of its group; the other slots are padding.
All inputs are finite; a program needn't handle non-finite values.
Results may differ from the reference program's by a relative error of at most 0.0046.
Values may be sent and summed in bfloat16 or wider, within the bound.
A program may use at most 128 MiB of HBM per device.

```python
import jax
import jax.numpy as jnp
from jax import lax

D = 3072
FF = 12288
SEQ_GRP = 8
GROUP_TOK = 640
TOKENS = 1280
MAX_LEN = 80
SEQS = 16
N_REP = 2
N_MP = 16


def packed_layout(base):
    drawn = jax.random.randint(base, (N_REP, SEQ_GRP), MAX_LEN // 4, MAX_LEN + 1)
    longest = jax.random.randint(jax.random.fold_in(base, 1), (N_REP,), 0, SEQ_GRP)
    column = jnp.arange(SEQ_GRP, dtype=jnp.int32)
    drawn = jnp.where(column[None, :] == longest[:, None], MAX_LEN, drawn).astype(jnp.int32)
    spare = (MAX_LEN - drawn + 1).astype(jnp.int32)
    shift_bits = jax.random.randint(jax.random.fold_in(base, 2), (N_REP, SEQ_GRP), 0, 1 << 20)
    shift = (shift_bits % spare).astype(jnp.int32)
    starts = (column[None, :] * MAX_LEN + shift).astype(jnp.int32)
    return (drawn.reshape(-1), starts.reshape(-1))


def draw_lengths(key, part):
    return packed_layout(jax.random.fold_in(key, 7))[0]


def draw_offsets(key, part):
    return packed_layout(jax.random.fold_in(key, 7))[1]


def with_ends(array, key, smallest, top_value):
    place = [jax.random.randint(jax.random.fold_in(key, axis), (), 0, length) for axis, length in enumerate(array.shape)]
    main_axis = array.shape.index(max(array.shape))
    beside = place[:main_axis] + [(place[main_axis] + 1) % array.shape[main_axis]] + place[main_axis + 1:]
    return array.at[tuple(place)].set(smallest).at[tuple(beside)].set(top_value)


def block_scale(rng, shape, pieces, low, top_value):
    def one(position, parts):
        heights = jax.random.uniform(jax.random.fold_in(jax.random.fold_in(rng, 6), position), (parts,), jnp.float32, low / len(pieces), top_value / len(pieces))
        return jnp.repeat(jnp.exp(heights), shape[position] // parts).reshape((-1,) + (1,) * (len(shape) - position - 1))

    factor_of = one(*pieces[0])
    for cut in pieces[1:]:
        factor_of = factor_of * one(*cut)
    return factor_of


def bell_draw(key, shape, spread, bound, shards=(), held_as=jnp.bfloat16):
    loudness = block_scale(key, shape, shards, -0.22, 0.18) if shards else 1.0
    values = jax.random.normal(key, shape, jnp.float32) * spread * loudness
    return jnp.minimum(jnp.maximum(values, -bound), bound).astype(held_as)


def setup_inputs(seed: int = 0) -> dict:
    keys = jax.random.split(jax.random.key(seed), 10)
    tokens = bell_draw(keys[0], (TOKENS, D), 1.0, 6.0, ((0, 32),))
    w_in = bell_draw(keys[1], (N_REP, D, 2, FF), D ** -0.5, 0.109375, ((0, 2), (3, 16)))
    w_down = bell_draw(keys[2], (N_REP, FF, D), FF ** -0.5, 0.0546875, ((0, 2), (1, 16)))
    norm_gain = jnp.clip(1.0 + 0.18 * jax.random.normal(keys[3], (D,), jnp.float32), 0.1, 1.9)
    final_gain = jnp.clip(1.0 + 0.18 * jax.random.normal(keys[4], (D,), jnp.float32), 0.1, 1.9)
    value_head = bell_draw(keys[5], (D,), 0.1, 0.6, (), jnp.float32)
    owner = with_ends(jax.random.randint(keys[6], (N_MP,), 0, N_REP), jax.random.fold_in(keys[6], 1), 0, N_REP - 1).astype(jnp.int32)
    lengths = draw_lengths(jax.random.fold_in(keys[9], 71), 0)
    offsets = draw_offsets(jax.random.fold_in(keys[9], 71), 0)
    return dict(tokens=tokens, w_in=w_in, w_down=w_down, norm_gain=norm_gain, final_gain=final_gain, value_head=value_head, owner=owner, lengths=lengths, offsets=offsets)


def reference(tokens, w_in, w_down, norm_gain, final_gain, value_head, owner, lengths, offsets):
    shard_cols = FF // N_MP
    shard_ids = jnp.arange(N_MP, dtype=jnp.int32)
    inner_split = w_in.reshape(N_REP, D, 2, N_MP, shard_cols)
    inner_chosen = jnp.transpose(inner_split[owner, :, :, shard_ids, :], (1, 2, 0, 3)).reshape(D, 2, FF)
    gate_weight = inner_chosen[:, 0, :]
    up_weight = inner_chosen[:, 1, :]
    down_weight = w_down.reshape(N_REP, N_MP, shard_cols, D)[owner, shard_ids].reshape(FF, D)
    grouped = tokens.reshape(N_REP, GROUP_TOK, D)
    group_lengths = lengths.reshape(N_REP, SEQ_GRP)
    group_offsets = offsets.reshape(N_REP, SEQ_GRP)

    def one_group(packed):
        block, seq_lengths, seq_offsets = packed
        slots = jnp.arange(GROUP_TOK, dtype=jnp.int32)
        member = ((slots[:, None] >= seq_offsets[None, :]) & (slots[:, None] < seq_offsets[None, :] + seq_lengths[None, :])).astype(jnp.float32)
        live = lax.optimization_barrier(jnp.sum(member, axis=1))
        block_f = block.astype(jnp.float32)
        normed = (block_f * lax.rsqrt(lax.optimization_barrier(jnp.mean(block_f * block_f, axis=1, keepdims=True)) + 1e-06) * norm_gain).astype(jnp.bfloat16)
        gate_part = jnp.dot(normed, gate_weight, preferred_element_type=jnp.float32)
        up_part = jnp.dot(normed, up_weight, preferred_element_type=jnp.float32)
        hidden = (jax.nn.gelu(gate_part, approximate=True) * up_part * live[:, None]).astype(jnp.bfloat16)
        resid = block_f + jnp.dot(hidden, down_weight, preferred_element_type=jnp.float32)
        final = resid * lax.rsqrt(lax.optimization_barrier(jnp.mean(resid * resid, axis=1, keepdims=True)) + 1e-06) * final_gain
        values = jnp.dot(final, value_head, precision=lax.Precision.HIGHEST)
        totals = jnp.dot(values, member, precision=lax.Precision.HIGHEST)
        return (resid.astype(jnp.bfloat16), totals / seq_lengths.astype(jnp.float32))
    mixed, rewards = lax.map(one_group, (grouped, group_lengths, group_offsets))
    return (mixed.reshape(TOKENS, D), rewards.reshape(SEQS))
```

```python
import functools

import jax
import jax.numpy as jnp
from jax import lax
from jax.experimental import pallas as pl
from jax.experimental.pallas import tpu as pltpu
from jax.sharding import PartitionSpec as P


def spread(value, axis, source):
    kept = jnp.where(lax.axis_index(axis) == source, value, 0).astype(value.dtype)
    return lax.psum(kept, axis)


def membership(slots, lengths, offsets):
    inside = (slots[:, None] >= offsets[None, :]) & (
        slots[:, None] < offsets[None, :] + lengths[None, :]
    )
    return inside.astype(jnp.float32)


def norm_rows(tokens_f, norm_gain):
    return (
        tokens_f
        * lax.rsqrt(jnp.mean(tokens_f * tokens_f, axis=1, keepdims=True) + 1e-06)
        * norm_gain
    ).astype(jnp.bfloat16)


def finish(tokens_f, delta, final_gain, value_head, lengths, offsets):
    tok_rows = tokens_f.shape[0]
    resid = tokens_f + delta
    mixed = resid.astype(jnp.bfloat16)
    final = resid * lax.rsqrt(jnp.mean(resid * resid, axis=1, keepdims=True) + 1e-06) * final_gain
    values = jnp.dot(final, value_head, precision=lax.Precision.HIGHEST)
    own_slots = lax.axis_index("mp") * tok_rows + jnp.arange(tok_rows, dtype=jnp.int32)
    member = membership(own_slots, lengths, offsets)
    partial_sums = jnp.dot(values, member, precision=lax.Precision.HIGHEST)
    totals = lax.psum(partial_sums, "mp")
    rewards = totals / lengths.astype(jnp.float32)
    return (mixed, rewards)


def move_weights(tokens, w_in, w_down, norm_gain, final_gain, value_head, owner, lengths, offsets):
    owner_index = owner[0]
    width = tokens.shape[1]
    hidden_cols = w_in.shape[3]
    tokens_f = tokens.astype(jnp.float32)
    normed = norm_rows(tokens_f, norm_gain)
    inner_local, outer_local = (
        spread(w_in, "rep", owner_index),
        spread(w_down, "rep", owner_index),
    )
    inner_matrix = inner_local.reshape(width, 2 * hidden_cols)
    piece = lax.all_gather(normed, "mp", axis=0, tiled=True)
    slots = jnp.arange(piece.shape[0], dtype=jnp.int32)
    row_count = piece.shape[0]
    products = jnp.dot(piece, inner_matrix, preferred_element_type=jnp.float32).reshape(
        row_count, 2, hidden_cols
    )
    gate_part = products[:, 0, :]
    up_part = products[:, 1, :]
    hidden = (
        jax.nn.gelu(gate_part, approximate=True)
        * up_part
        * jnp.sum(membership(slots, lengths, offsets), axis=1)[:, None]
    ).astype(jnp.bfloat16)
    outer_matrix = outer_local.reshape(hidden_cols, width)
    delta = lax.psum_scatter(
        jnp.dot(hidden, outer_matrix, preferred_element_type=jnp.float32),
        "mp",
        scatter_dimension=0,
        tiled=True,
    )
    return finish(tokens_f, delta, final_gain, value_head, lengths, offsets)


MESH = pl.DeviceIdType.MESH


def mega_kernel(levels, tok_ref, gain_ref, mine_ref, live_ref, member_ref, final_ref, head_ref, win_ref, wdown_ref,
                mixed_ref, totals_ref,
                x_buf, part, swap_buf, sum_buf, cross_buf, first_buf, second_buf, level_buf, win, wdown, hid,
                nrm, stage, acc, delta, mean_buf, own_mean,
                w_sem, half_send, half_recv, level_send, first_send, second_send, cross_send, pass_send, recv_sem,
                swap_send, swap_recv, sum_send, cross_recv, first_recv, second_recv, level_recv, back_send, back_recv,
                mean_send, mean_recv):
    rep, slot = lax.axis_index("rep"), lax.axis_index("mp")
    side, row, level = slot % 2, (slot // 2) % 2, slot // 4
    parts = levels * 4
    other_rep, other_row, twin = 1 - rep, 1 - row, 1 - side
    here, cross = (rep, row), (other_rep, other_row)
    first = (rep * side + other_rep * twin, row * twin + other_row * side)
    second = (rep * twin + other_rep * side, row * side + other_row * twin)
    tok_rows, width = tok_ref.shape
    rows, half = 2 * tok_rows, width // 2
    cols = wdown.shape[0]

    def index_of(column, at):
        return at * 4 + column[0] * 2 + column[1]

    def remote(src, dst, send_sem, recv_sem, column, at, plane):
        return pltpu.make_async_remote_copy(
            src_ref=src, dst_ref=dst, send_sem=send_sem, recv_sem=recv_sem,
            device_id=(column[0], at * 4 + column[1] * 2 + plane), device_id_type=MESH,
        )

    barrier = pltpu.get_barrier_semaphore()
    pl.semaphore_signal(barrier, inc=1, device_id=(other_rep, slot), device_id_type=MESH)

    @pl.loop(1, parts)
    def _(d):
        pl.semaphore_signal(barrier, inc=1, device_id=(rep, (slot + d) % parts), device_id_type=MESH)

    load_in = pltpu.make_async_copy(win_ref, win, w_sem.at[0])
    load_down = pltpu.make_async_copy(wdown_ref, wdown, w_sem.at[1])
    load_in.start()
    load_down.start()

    mine = index_of(here, level)
    my_rows = pl.ds(pl.multiple_of(side * tok_rows, 8), tok_rows)
    twin_rows = pl.ds(pl.multiple_of(twin * tok_rows, 8), tok_rows)
    my_cols = pl.ds(pl.multiple_of(side * half, 128), half)
    twin_cols = pl.ds(pl.multiple_of(twin * half, 128), half)

    tok = tok_ref[...].astype(jnp.float32)
    nrm[...] = tok * lax.rsqrt(jnp.mean(tok * tok, axis=1, keepdims=True) + 1e-06) * gain_ref[...]

    pl.semaphore_wait(barrier, parts)

    trade = remote(nrm.at[:, twin_cols], stage.at[my_rows], half_send, half_recv, here, level, twin)
    trade.start()
    stage[my_rows, :] = nrm[:, my_cols]
    trade.wait_recv()
    x_buf[side, mine] = stage[...].astype(jnp.bfloat16)

    def from_level(d):
        return (level + levels - d) % levels

    def piece(index):
        return x_buf.at[side, index]

    def move(index, sem, column, at):
        return remote(piece(index), piece(index), sem, recv_sem.at[side, index], column, at, side)

    def climb(d):
        return move(mine, level_send.at[d], here, (level + d) % levels)

    def hand(index):
        return remote(piece(index), piece(index), pass_send.at[index], recv_sem.at[side, index], here, level, twin)

    def arrive(plane, index):
        pltpu.make_async_copy(x_buf.at[plane, index], x_buf.at[plane, index], recv_sem.at[plane, index]).wait()

    move(mine, first_send.at[0], first, level).start()
    move(mine, second_send.at[0], second, level).start()

    @pl.loop(1, levels)
    def _(d):
        climb(d).start()

    hand(mine).start()

    def relay(d):
        index = index_of(first, from_level(d))
        arrive(side, index)
        move(index, cross_send.at[d], second, level).start()
        hand(index).start()

    def descend(d):
        index = index_of(here, from_level(d))
        arrive(side, index)
        move(index, first_send.at[d], first, level).start()
        move(index, second_send.at[d], second, level).start()
        hand(index).start()

    def settle(d):
        for column in (second, cross):
            index = index_of(column, from_level(d))
            arrive(side, index)
            hand(index).start()

    def collect_hands(d):
        for column in (here, first, second, cross):
            arrive(twin, index_of(column, from_level(d)))

    def at_level(buf, plane, at):
        return buf[plane, pl.ds(at * 4, 4)]

    up_block = 256

    def up(d):
        at = from_level(d)

        @pl.loop(0, cols // up_block)
        def _(n):
            lo = pl.multiple_of(n * up_block, up_block)

            def dot(offset):
                span = pl.ds(lo + offset, up_block)
                left = at_level(x_buf, 0, at).reshape(4 * rows, half)
                right = at_level(x_buf, 1, at).reshape(4 * rows, half)
                return (jnp.dot(left, win[:half, span], preferred_element_type=jnp.float32)
                        + jnp.dot(right, win[half:, span], preferred_element_type=jnp.float32))

            gate, lift = dot(0), dot(cols)
            hid[:, pl.ds(lo, up_block)] = (
                jax.nn.gelu(gate, approximate=True) * lift * mine_ref[...]
            ).astype(jnp.bfloat16)

    down_block = 512

    def down(d, plane):
        at = from_level(d)

        @pl.loop(0, half // down_block)
        def _(n):
            lo = pl.multiple_of(n * down_block, down_block)
            out = jnp.dot(hid[...], wdown[:, pl.ds(pl.multiple_of(plane * half + lo, down_block), down_block)],
                          preferred_element_type=jnp.float32)
            part[plane, pl.ds(at * 4, 4), :, pl.ds(lo, down_block)] = out.astype(jnp.bfloat16).reshape(
                4, rows, down_block)

    def swap(index):
        return remote(part.at[twin, index], swap_buf.at[index], swap_send.at[index], swap_recv.at[index], here, level, twin)

    def send(index, buf, sem, at, column, to):
        return remote(sum_buf.at[index], buf.at[at], sum_send.at[index], sem.at[at], column, to, side)

    def landed(buf, sem, at):
        pltpu.make_async_copy(buf.at[at], buf.at[at], sem.at[at]).wait()

    def both(index):
        swap(index).wait_recv()
        return part[side, index].astype(jnp.float32) + swap_buf[index].astype(jnp.float32)

    def start_swaps(d):
        for column in (cross, second, first, here):
            swap(index_of(column, from_level(d))).start()

    def reduce_outer(d):
        at = from_level(d)
        for column, buf, sem in ((cross, cross_buf, cross_recv), (second, second_buf, second_recv)):
            index = index_of(column, at)
            sum_buf[index] = both(index).astype(jnp.bfloat16)
            send(index, buf, sem, at, second, level).start()

    def reduce_first(d):
        at = from_level(d)
        index = index_of(first, at)
        total = both(index)
        landed(cross_buf, cross_recv, at)
        sum_buf[index] = (total + cross_buf[at].astype(jnp.float32)).astype(jnp.bfloat16)
        send(index, first_buf, first_recv, at, first, level).start()

    def reduce_here(d):
        at = from_level(d)
        index = index_of(here, at)
        total = both(index)
        landed(second_buf, second_recv, at)
        landed(first_buf, first_recv, at)
        total = total + (second_buf[at].astype(jnp.float32) + first_buf[at].astype(jnp.float32))
        if d == 0:
            acc[...] = total
        else:
            sum_buf[index] = total.astype(jnp.bfloat16)
            send(index, level_buf, level_recv, level, here, at).start()

    relay(0)
    descend(1)
    settle(0)
    collect_hands(0)
    load_in.wait()
    load_down.wait()

    for d in range(levels):
        up(d)
        if d + 1 < levels:
            relay(d + 1)
        if d + 2 < levels:
            descend(d + 2)
        if d >= 1:
            reduce_first(d - 1)
        if d >= 2:
            reduce_here(d - 2)
        down(d, twin)
        start_swaps(d)
        down(d, side)
        if d + 1 < levels:
            settle(d + 1)
        reduce_outer(d)
        if d + 1 < levels:
            collect_hands(d + 1)

    if levels >= 2:
        reduce_here(levels - 2)
    reduce_first(levels - 1)
    reduce_here(levels - 1)

    @pl.loop(1, levels)
    def _(d):
        at = (level + d) % levels
        landed(level_buf, level_recv, at)
        acc[...] += level_buf[at].astype(jnp.float32)

    back = remote(acc.at[twin_rows], delta.at[:, my_cols], back_send, back_recv, here, level, twin)
    back.start()
    delta[:, my_cols] = acc[my_rows, :]
    back.wait_recv()
    resid = tok_ref[...].astype(jnp.float32) + delta[...] * live_ref[...]
    mixed_ref[...] = resid.astype(jnp.bfloat16)
    scale = lax.rsqrt(jnp.mean(resid * resid, axis=1, keepdims=True) + 1e-06)
    values = jnp.sum(resid * scale * final_ref[...] * head_ref[...], axis=1, keepdims=True)
    own_mean[...] = jnp.broadcast_to(jnp.sum(values * member_ref[...], axis=0, keepdims=True), own_mean.shape)

    def tell(d):
        to = (slot + d) % parts
        return pltpu.make_async_remote_copy(
            src_ref=own_mean, dst_ref=mean_buf.at[slot], send_sem=mean_send.at[to],
            recv_sem=mean_recv.at[slot], device_id=(rep, to), device_id_type=MESH,
        )

    @pl.loop(1, parts)
    def _(d):
        tell(d).start()

    totals_ref[...] = own_mean[...]

    trade.wait_send()
    back.wait_send()

    @pl.loop(0, levels)
    def _(d):
        for sem in (first_send, second_send, cross_send):
            move(mine, sem.at[d], first, level).wait_send()

    @pl.loop(1, levels)
    def _(d):
        climb(d).wait_send()

    @pl.loop(0, parts)
    def _(i):
        hand(i).wait_send()
        swap(i).wait_send()

    @pl.loop(0, levels)
    def _(d):
        for column in (cross, second, first):
            send(index_of(column, d), cross_buf, cross_recv, level, second, level).wait_send()

    @pl.loop(1, levels)
    def _(d):
        send(index_of(here, from_level(d)), level_buf, level_recv, level, second, level).wait_send()

    @pl.loop(1, parts)
    def _(d):
        index = (slot + parts - d) % parts
        pltpu.make_async_copy(own_mean, mean_buf.at[index], mean_recv.at[index]).wait()
        totals_ref[...] += mean_buf[index]

    @pl.loop(1, parts)
    def _(d):
        tell(d).wait_send()


def mega_rows(reps, parts, tokens, w_in, w_down, norm_gain, final_gain, value_head, owner, lengths, offsets):
    tok_rows, width = tokens.shape
    cols = w_in.shape[3]
    levels, half, rows = parts // 4, width // 2, 2 * tok_rows
    own_slots = lax.axis_index("mp") * tok_rows + jnp.arange(tok_rows, dtype=jnp.int32)
    member = membership(own_slots, lengths, offsets)
    live = jnp.sum(member, axis=1)[:, None]
    count = lengths.shape[0]
    member = jnp.pad(member, ((0, 0), (0, 128 - count)))
    mine = jnp.broadcast_to((owner == lax.axis_index("rep")).astype(jnp.float32)[:, None], (1, 256))
    vmem = pl.BlockSpec(memory_space=pltpu.VMEM)
    hbm = pl.BlockSpec(memory_space=pl.ANY)
    dma = pltpu.SemaphoreType.DMA
    chips = parts
    f32, bf16 = jnp.float32, jnp.bfloat16

    def units(count):
        return pltpu.VMEM((count, rows, half), bf16)

    mixed, totals = pl.pallas_call(
        functools.partial(mega_kernel, levels),
        out_shape=(
            jax.ShapeDtypeStruct((tok_rows, width), bf16),
            jax.ShapeDtypeStruct((8, 128), f32),
        ),
        in_specs=[vmem] * 7 + [hbm] * 2,
        out_specs=(vmem, vmem),
        scratch_shapes=[
            pltpu.VMEM((2, chips, rows, half), bf16),
            pltpu.VMEM((2, chips, rows, half), bf16),
            units(chips), units(chips), units(levels), units(levels), units(levels), units(levels),
            pltpu.VMEM((width, 2 * cols), bf16),
            pltpu.VMEM((cols, width), bf16),
            pltpu.VMEM((4 * rows, cols), bf16),
            pltpu.VMEM((tok_rows, width), f32),
            pltpu.VMEM((rows, half), f32),
            pltpu.VMEM((rows, half), f32),
            pltpu.VMEM((tok_rows, width), f32),
            pltpu.VMEM((parts, 8, 128), f32),
            pltpu.VMEM((8, 128), f32),
            dma((2,)), dma, dma,
            dma((levels,)), dma((levels,)), dma((levels,)), dma((levels,)), dma((chips,)), dma((2, chips)),
            dma((chips,)), dma((chips,)), dma((chips,)),
            dma((levels,)), dma((levels,)), dma((levels,)), dma((levels,)), dma, dma,
            dma((parts,)), dma((parts,)),
        ],
        compiler_params=pltpu.CompilerParams(
            collective_id=0, has_side_effects=True, vmem_limit_bytes=60 << 20
        ),
    )(tokens, norm_gain[None, :], mine, live, member, final_gain[None, :], value_head[None, :],
      w_in.reshape(width, 2 * cols), w_down[0])
    return mixed, totals[0, :count] / lengths.astype(f32)


def per_device(reps, parts, *args):
    tokens, w_in, w_down = args[:3]
    tok_rows, width = tokens.shape
    cols = w_in.shape[3]
    row_bytes = 2 * reps * parts * tokens.size * 2
    weight_bytes = 2 * (w_in.size + w_down.size)
    fits = tok_rows % 8 == 0 and width % 1024 == 0 and cols % 256 == 0 and args[7].shape[0] <= 128
    if reps == 2 and parts == 16 and fits and row_bytes < 2 * weight_bytes:
        return mega_rows(reps, parts, *args)
    return move_weights(*args)


def solution(mesh):
    in_specs = (
        P(("rep", "mp"), None),
        P("rep", None, None, "mp"),
        P("rep", "mp", None),
        P(),
        P(),
        P(),
        P("mp"),
        P("rep"),
        P("rep"),
    )
    out_specs = (P(("rep", "mp"), None), P("rep"))
    return jax.shard_map(
        functools.partial(per_device, mesh.shape["rep"], mesh.shape["mp"]),
        mesh=mesh, in_specs=in_specs, out_specs=out_specs, check_vma=False,
    )
```

```python
import functools

import jax
import jax.numpy as jnp
from jax import lax
from jax.experimental import pallas as pl
from jax.experimental.pallas import tpu as pltpu
from jax.sharding import PartitionSpec as P


def spread(value, axis, source):
    kept = jnp.where(lax.axis_index(axis) == source, value, 0).astype(value.dtype)
    return lax.psum(kept, axis)


def membership(slots, lengths, offsets):
    inside = (slots[:, None] >= offsets[None, :]) & (
        slots[:, None] < offsets[None, :] + lengths[None, :]
    )
    return inside.astype(jnp.float32)


def norm_rows(tokens_f, norm_gain):
    return (
        tokens_f
        * lax.rsqrt(jnp.mean(tokens_f * tokens_f, axis=1, keepdims=True) + 1e-06)
        * norm_gain
    ).astype(jnp.bfloat16)


def finish(tokens_f, delta, final_gain, value_head, lengths, offsets):
    tok_rows = tokens_f.shape[0]
    resid = tokens_f + delta
    mixed = resid.astype(jnp.bfloat16)
    final = resid * lax.rsqrt(jnp.mean(resid * resid, axis=1, keepdims=True) + 1e-06) * final_gain
    values = jnp.dot(final, value_head, precision=lax.Precision.HIGHEST)
    own_slots = lax.axis_index("mp") * tok_rows + jnp.arange(tok_rows, dtype=jnp.int32)
    member = membership(own_slots, lengths, offsets)
    partial_sums = jnp.dot(values, member, precision=lax.Precision.HIGHEST)
    totals = lax.psum(partial_sums, "mp")
    rewards = totals / lengths.astype(jnp.float32)
    return (mixed, rewards)


def move_weights(tokens, w_in, w_down, norm_gain, final_gain, value_head, owner, lengths, offsets):
    owner_index = owner[0]
    width = tokens.shape[1]
    hidden_cols = w_in.shape[3]
    tokens_f = tokens.astype(jnp.float32)
    normed = norm_rows(tokens_f, norm_gain)
    inner_local, outer_local = (
        spread(w_in, "rep", owner_index),
        spread(w_down, "rep", owner_index),
    )
    inner_matrix = inner_local.reshape(width, 2 * hidden_cols)
    piece = lax.all_gather(normed, "mp", axis=0, tiled=True)
    slots = jnp.arange(piece.shape[0], dtype=jnp.int32)
    row_count = piece.shape[0]
    products = jnp.dot(piece, inner_matrix, preferred_element_type=jnp.float32).reshape(
        row_count, 2, hidden_cols
    )
    gate_part = products[:, 0, :]
    up_part = products[:, 1, :]
    hidden = (
        jax.nn.gelu(gate_part, approximate=True)
        * up_part
        * jnp.sum(membership(slots, lengths, offsets), axis=1)[:, None]
    ).astype(jnp.bfloat16)
    outer_matrix = outer_local.reshape(hidden_cols, width)
    delta = lax.psum_scatter(
        jnp.dot(hidden, outer_matrix, preferred_element_type=jnp.float32),
        "mp",
        scatter_dimension=0,
        tiled=True,
    )
    return finish(tokens_f, delta, final_gain, value_head, lengths, offsets)


MESH = pl.DeviceIdType.MESH


def mega_kernel(levels, cuts, tok_ref, gain_ref, final_ref, head_ref, owner_ref, lengths_ref, offsets_ref, win_ref,
                wdown_ref, mixed_ref, rewards_ref,
                x_buf, part, swap_buf, cross_buf, first_buf, second_buf, level_buf, raw, win, wdown, hid,
                acc, mean_buf, own_mean,
                w_sem, up_send, down_send, first_send, second_send, pass_send, recv_sem,
                swap_send, swap_recv, sum_send, cross_recv, first_recv, second_recv, level_recv,
                mean_send, mean_recv):
    rep, slot = lax.axis_index("rep"), lax.axis_index("mp")
    side, row, level = slot % 2, (slot // 2) % 2, slot // 4
    parts = levels * 4
    other_rep, other_row, twin = 1 - rep, 1 - row, 1 - side
    here, cross = (rep, row), (other_rep, other_row)
    first = (rep * side + other_rep * twin, row * twin + other_row * side)
    second = (rep * twin + other_rep * side, row * side + other_row * twin)
    tok_rows, width = tok_ref.shape
    cols, count = wdown.shape[0], lengths_ref.shape[1]
    cut = width // cuts

    def index_of(column, at):
        return at * 4 + column[0] * 2 + column[1]

    def remote(src, dst, send_sem, recv_sem, column, at, plane):
        return pltpu.make_async_remote_copy(
            src_ref=src, dst_ref=dst, send_sem=send_sem, recv_sem=recv_sem,
            device_id=(column[0], at * 4 + column[1] * 2 + plane), device_id_type=MESH,
        )

    barrier = pltpu.get_barrier_semaphore()
    pl.semaphore_signal(barrier, inc=1, device_id=(other_rep, slot), device_id_type=MESH)
    pl.semaphore_signal(barrier, inc=1, device_id=(rep, level * 4 + other_row * 2 + side), device_id_type=MESH)
    pl.semaphore_signal(barrier, inc=1, device_id=(rep, level * 4 + row * 2 + twin), device_id_type=MESH)

    @pl.loop(1, levels)
    def _(d):
        pl.semaphore_signal(barrier, inc=1, device_id=(rep, (slot + 4 * d) % parts), device_id_type=MESH)

    shares = 3
    share = width // shares

    def load_in(i):
        at = pl.ds(i * share, share)
        return pltpu.make_async_copy(win_ref.at[at], raw.at[at], w_sem.at[i])

    load_down = pltpu.make_async_copy(wdown_ref, wdown, w_sem.at[shares])
    for i in range(shares):
        load_in(i).start()
    load_down.start()

    block = 128

    def untangle(i):
        load_in(i).wait()
        to = lax.broadcasted_iota(jnp.int32, (2 * block, 2 * block), 0)
        at = lax.broadcasted_iota(jnp.int32, (2 * block, 2 * block), 1)
        pick = jnp.where((at == 2 * to) | (at == 2 * (to - block) + 1), 1.0, 0.0).astype(jnp.bfloat16)

        @pl.loop(0, share // block, unroll=2)
        def _(k):
            rows_at = pl.ds(pl.multiple_of(i * share + k * block, block), block)
            both_parts = jnp.dot(
                pick, raw[rows_at].reshape(2 * block, cols), preferred_element_type=jnp.float32
            ).astype(jnp.bfloat16)
            win[rows_at, :cols] = both_parts[:block]
            win[rows_at, cols:] = both_parts[block:]

    mine = index_of(here, level)
    tok = tok_ref[...].astype(jnp.float32)
    x_buf[mine, side] = (
        tok * lax.rsqrt(jnp.mean(tok * tok, axis=1, keepdims=True) + 1e-06) * gain_ref[...]
    ).astype(jnp.bfloat16)

    low = level < levels // 2
    inner = (level > 0) & (level < levels - 1)
    outer = jnp.logical_not(inner)

    def from_level(d):
        near = jnp.where(inner & (d < 2), 1 - d, d)
        return jnp.where(low, near, levels - 1 - near)

    def piece(index):
        return x_buf.at[index, side]

    def move(index, sem, column, at):
        return remote(piece(index), piece(index), sem, recv_sem.at[side, index], column, at, side)

    def hand(index):
        return remote(piece(index), piece(index), pass_send.at[index], recv_sem.at[side, index], here, level, twin)

    def arrive(plane, index):
        pltpu.make_async_copy(x_buf.at[index, plane], x_buf.at[index, plane], recv_sem.at[plane, index]).wait()

    def pass_on(index, upward, downward):
        @pl.when(upward & (level < levels - 1))
        def _():
            move(index, up_send.at[index], here, level + 1).start()

        @pl.when(downward & (level > 0))
        def _():
            move(index, down_send.at[index], here, level - 1).start()

        move(index, second_send.at[index], second, level).start()
        hand(index).start()

    def take(column, d):
        at = from_level(d)
        index = index_of(column, at)
        arrive(side, index)
        pass_on(index, at <= level, at >= level)

    def take_level(d):
        take(here, d)
        take(first, d)

    def settle(d):
        for column in (second, cross):
            index = index_of(column, from_level(d))
            arrive(side, index)
            hand(index).start()

    def collect_hands(d):
        for column in (here, first, second, cross):
            arrive(twin, index_of(column, from_level(d)))

    up_block = 256

    def up(d, n):
        lo = n * up_block
        left = x_buf[pl.ds(from_level(d) * 4, 4)].reshape(8 * tok_rows, width)
        gate = jnp.dot(left, win[:, lo:lo + up_block], preferred_element_type=jnp.float32)
        lift = jnp.dot(left, win[:, cols + lo:cols + lo + up_block], preferred_element_type=jnp.float32)
        chosen = jnp.where(owner_ref[...] == rep, 1.0, 0.0)
        hid[:, lo:lo + up_block] = (jax.nn.gelu(gate, approximate=True) * lift * chosen).astype(jnp.bfloat16)

    down_block = 512

    def down(d, q):
        at = from_level(d)

        @pl.loop(0, cut // down_block)
        def _(n):
            lo = pl.multiple_of(n * down_block, down_block)
            out = jnp.dot(hid[...], wdown[:, pl.ds(q * cut + lo, down_block)], preferred_element_type=jnp.float32)
            part[q, pl.ds(at * 4, 4), :, :, pl.ds(lo, down_block)] = out.astype(jnp.bfloat16).reshape(
                4, 2, tok_rows, down_block)

        for column in (cross, second, first, here):
            swap(index_of(column, at), q).start()

    def swap(index, q):
        return remote(part.at[q, index, twin], swap_buf.at[q, index], swap_send.at[q, index],
                      swap_recv.at[q, index], here, level, twin)

    def send(index, q, buf, sem, at, column, to):
        return remote(swap_buf.at[q, index], buf.at[q, at], sum_send.at[q, index], sem.at[q, at], column, to, side)

    def landed(buf, sem, q, at):
        pltpu.make_async_copy(buf.at[q, at], buf.at[q, at], sem.at[q, at]).wait()

    def both(index, q):
        swap(index, q).wait_recv()
        return part[q, index, side].astype(jnp.float32) + swap_buf[q, index].astype(jnp.float32)

    def reduce_outer(d, q, column, buf, sem):
        at = from_level(d)
        index = index_of(column, at)
        swap_buf[q, index] = both(index, q).astype(jnp.bfloat16)
        send(index, q, buf, sem, at, second, level).start()

    def reduce_cross(d, q):
        reduce_outer(d, q, cross, cross_buf, cross_recv)

    def reduce_second(d, q):
        reduce_outer(d, q, second, second_buf, second_recv)

    def reduce_first(d, q):
        at = from_level(d)
        index = index_of(first, at)
        total = both(index, q)
        landed(cross_buf, cross_recv, q, at)
        swap_buf[q, index] = (total + cross_buf[q, at].astype(jnp.float32)).astype(jnp.bfloat16)
        send(index, q, first_buf, first_recv, at, first, level).start()

    def reduce_here(d, q):
        at = from_level(d)
        index = index_of(here, at)
        total = both(index, q)
        landed(second_buf, second_recv, q, at)
        landed(first_buf, first_recv, q, at)
        total = total + (second_buf[q, at].astype(jnp.float32) + first_buf[q, at].astype(jnp.float32))
        if d == 0:
            acc[:, q * cut:(q + 1) * cut] = total
        else:
            swap_buf[q, index] = total.astype(jnp.bfloat16)
            send(index, q, level_buf, level_recv, level, here, at).start()

    pl.semaphore_wait(barrier, 3 + levels - 1)
    always = level >= 0
    move(mine, first_send, first, level).start()
    pass_on(mine, always, always)
    for i in range(shares):
        untangle(i)

    take(first, 0)
    take_level(1)

    @pl.when(inner)
    def _():
        take_level(2)

    settle(0)
    collect_hands(0)
    load_down.wait()

    def all_cuts(step, d):
        for q in range(cuts):
            step(d, q)

    ups = cols // up_block

    def up_all(d, lo=0, hi=ups):
        for n in range(lo, hi):
            up(d, n)

    def down_all(d):
        all_cuts(down, d)

    up_all(0, 0, 2)

    @pl.when(inner)
    def _():
        take(here, 3)

    up_all(0, 2)

    @pl.when(inner)
    def _():
        take(first, 3)

    down_all(0)
    all_cuts(reduce_cross, 0)
    all_cuts(reduce_second, 0)
    settle(1)
    collect_hands(1)
    up_all(1, 0, 1)

    @pl.when(outer)
    def _():
        take(here, 2)

    up_all(1, 1)
    all_cuts(reduce_first, 0)
    down(1, 0)

    @pl.when(outer)
    def _():
        take(first, 2)

    for q in range(1, cuts):
        down(1, q)
    all_cuts(reduce_cross, 1)
    all_cuts(reduce_second, 1)
    all_cuts(reduce_here, 0)

    @pl.when(outer)
    def _():
        take(here, 3)

    settle(2)
    collect_hands(2)
    up_all(2)
    all_cuts(reduce_first, 1)

    @pl.when(outer)
    def _():
        take(first, 3)

    down_all(2)
    all_cuts(reduce_cross, 2)
    all_cuts(reduce_second, 2)
    all_cuts(reduce_here, 1)
    settle(3)
    collect_hands(3)
    up_all(3)
    all_cuts(reduce_first, 2)
    down_all(3)
    all_cuts(reduce_cross, 3)
    all_cuts(reduce_second, 3)
    all_cuts(reduce_here, 2)
    all_cuts(reduce_first, 3)
    all_cuts(reduce_here, 3)

    for q in range(cuts):
        @pl.loop(1, levels)
        def _(d):
            at = (level + d) % levels
            landed(level_buf, level_recv, q, at)
            acc[:, q * cut:(q + 1) * cut] += level_buf[q, at].astype(jnp.float32)

    own_slots = slot * tok_rows + lax.broadcasted_iota(jnp.int32, (tok_rows, count), 0)
    starts = offsets_ref[...]
    member = jnp.where((own_slots >= starts) & (own_slots < starts + lengths_ref[...]), 1.0, 0.0)
    live = jnp.sum(member, axis=1, keepdims=True)
    resid = tok_ref[...].astype(jnp.float32) + acc[...] * live
    scale = lax.rsqrt(jnp.mean(resid * resid, axis=1, keepdims=True) + 1e-06)
    values = jnp.sum(resid * scale * final_ref[...] * head_ref[...], axis=1, keepdims=True)
    own_mean[...] = jnp.broadcast_to(jnp.sum(values * member, axis=0, keepdims=True), own_mean.shape)

    def tell(d):
        to = (slot + d) % parts
        return pltpu.make_async_remote_copy(
            src_ref=own_mean, dst_ref=mean_buf.at[slot], send_sem=mean_send.at[to],
            recv_sem=mean_recv.at[slot], device_id=(rep, to), device_id_type=MESH,
        )

    @pl.loop(1, parts)
    def _(d):
        tell(d).start()

    mixed_ref[...] = resid.astype(jnp.bfloat16)
    acc[:8, :count] = own_mean[...]
    move(mine, first_send, first, level).wait_send()

    @pl.loop(0, levels)
    def _(d):
        for column in (here, first):
            index = index_of(column, d)
            move(index, second_send.at[index], second, level).wait_send()

            @pl.when((d <= level) & (level < levels - 1))
            def _():
                move(index, up_send.at[index], here, level).wait_send()

            @pl.when((d >= level) & (level > 0))
            def _():
                move(index, down_send.at[index], here, level).wait_send()

    @pl.loop(0, parts)
    def _(i):
        hand(i).wait_send()
        for q in range(cuts):
            swap(i, q).wait_send()

    @pl.loop(0, levels)
    def _(d):
        for q in range(cuts):
            for column in (cross, second, first):
                send(index_of(column, d), q, cross_buf, cross_recv, level, second, level).wait_send()

    @pl.loop(1, levels)
    def _(d):
        for q in range(cuts):
            send(index_of(here, (level + d) % levels), q, level_buf, level_recv, level, second, level).wait_send()

    @pl.loop(1, parts)
    def _(d):
        index = (slot + parts - d) % parts
        pltpu.make_async_copy(own_mean, mean_buf.at[index], mean_recv.at[index]).wait()
        acc[:8, :count] += mean_buf[index]

    rewards_ref[...] = acc[:1, :count] / lengths_ref[...].astype(jnp.float32)

    @pl.loop(1, parts)
    def _(d):
        tell(d).wait_send()


def mega_rows(reps, parts, tokens, w_in, w_down, norm_gain, final_gain, value_head, owner, lengths, offsets):
    tok_rows, width = tokens.shape
    cols = w_in.shape[3]
    levels, cuts = parts // 4, 2
    cut, count = width // cuts, lengths.shape[0]
    vmem = pl.BlockSpec(memory_space=pltpu.VMEM)
    hbm = pl.BlockSpec(memory_space=pl.ANY)
    dma = pltpu.SemaphoreType.DMA
    f32, bf16 = jnp.float32, jnp.bfloat16
    few = pltpu.VMEM((cuts, levels, tok_rows, cut), bf16)
    some, each = dma((cuts, levels)), dma((cuts, parts))
    mixed, rewards = pl.pallas_call(
        functools.partial(mega_kernel, levels, cuts),
        out_shape=(
            jax.ShapeDtypeStruct((tok_rows, width), bf16),
            jax.ShapeDtypeStruct((1, count), f32),
        ),
        in_specs=[vmem] * 7 + [hbm] * 2,
        out_specs=(vmem, vmem),
        scratch_shapes=[
            pltpu.VMEM((parts, 2, tok_rows, width), bf16),
            pltpu.VMEM((cuts, parts, 2, tok_rows, cut), bf16),
            pltpu.VMEM((cuts, parts, tok_rows, cut), bf16),
            few, few, few, few,
            pltpu.VMEM((width, 2, cols), bf16),
            pltpu.VMEM((width, 2 * cols), bf16),
            pltpu.VMEM((cols, width), bf16),
            pltpu.VMEM((8 * tok_rows, cols), bf16),
            pltpu.VMEM((tok_rows, width), f32),
            pltpu.VMEM((parts, 8, count), f32),
            pltpu.VMEM((8, count), f32),
            dma((4,)), dma((parts,)), dma((parts,)), dma, dma((parts,)), dma((parts,)), dma((2, parts)),
            each, each, each, some, some, some, some,
            dma((parts,)), dma((parts,)),
        ],
        compiler_params=pltpu.CompilerParams(
            collective_id=0, has_side_effects=True, vmem_limit_bytes=54 << 20
        ),
    )(tokens, norm_gain[None, :], final_gain[None, :], value_head[None, :], owner[None, :], lengths[None, :],
      offsets[None, :], w_in[0], w_down[0])
    return mixed, rewards[0]


def per_device(reps, parts, *args):
    tokens, w_in, w_down = args[:3]
    tok_rows, width = tokens.shape
    cols = w_in.shape[3]
    row_bytes = 2 * reps * parts * tokens.size * 2
    weight_bytes = 2 * (w_in.size + w_down.size)
    fits = tok_rows % 8 == 0 and width % 3072 == 0 and cols % 256 == 0 and args[7].shape[0] <= 128
    if reps == 2 and parts == 16 and fits and row_bytes < 2 * weight_bytes:
        return mega_rows(reps, parts, *args)
    return move_weights(*args)


def solution(mesh):
    in_specs = (
        P(("rep", "mp"), None),
        P("rep", None, None, "mp"),
        P("rep", "mp", None),
        P(),
        P(),
        P(),
        P("mp"),
        P("rep"),
        P("rep"),
    )
    out_specs = (P(("rep", "mp"), None), P("rep"))
    return jax.shard_map(
        functools.partial(per_device, mesh.shape["rep"], mesh.shape["mp"]),
        mesh=mesh, in_specs=in_specs, out_specs=out_specs, check_vma=False,
    )
```

```python
import functools

import jax
import jax.numpy as jnp
from jax import lax
from jax.experimental import pallas as pl
from jax.experimental.pallas import tpu as pltpu
from jax.sharding import PartitionSpec as P


def spread(value, axis, source):
    kept = jnp.where(lax.axis_index(axis) == source, value, 0).astype(value.dtype)
    return lax.psum(kept, axis)


def membership(slots, lengths, offsets):
    inside = (slots[:, None] >= offsets[None, :]) & (
        slots[:, None] < offsets[None, :] + lengths[None, :]
    )
    return inside.astype(jnp.float32)


def norm_rows(tokens_f, norm_gain):
    return (
        tokens_f
        * lax.rsqrt(jnp.mean(tokens_f * tokens_f, axis=1, keepdims=True) + 1e-06)
        * norm_gain
    ).astype(jnp.bfloat16)


def finish(tokens_f, delta, final_gain, value_head, lengths, offsets):
    tok_rows = tokens_f.shape[0]
    resid = tokens_f + delta
    mixed = resid.astype(jnp.bfloat16)
    final = resid * lax.rsqrt(jnp.mean(resid * resid, axis=1, keepdims=True) + 1e-06) * final_gain
    values = jnp.dot(final, value_head, precision=lax.Precision.HIGHEST)
    own_slots = lax.axis_index("mp") * tok_rows + jnp.arange(tok_rows, dtype=jnp.int32)
    member = membership(own_slots, lengths, offsets)
    partial_sums = jnp.dot(values, member, precision=lax.Precision.HIGHEST)
    totals = lax.psum(partial_sums, "mp")
    rewards = totals / lengths.astype(jnp.float32)
    return (mixed, rewards)


def move_weights(tokens, w_in, w_down, norm_gain, final_gain, value_head, owner, lengths, offsets):
    owner_index = owner[0]
    width = tokens.shape[1]
    hidden_cols = w_in.shape[3]
    tokens_f = tokens.astype(jnp.float32)
    normed = norm_rows(tokens_f, norm_gain)
    inner_local, outer_local = (
        spread(w_in, "rep", owner_index),
        spread(w_down, "rep", owner_index),
    )
    inner_matrix = inner_local.reshape(width, 2 * hidden_cols)
    piece = lax.all_gather(normed, "mp", axis=0, tiled=True)
    slots = jnp.arange(piece.shape[0], dtype=jnp.int32)
    row_count = piece.shape[0]
    products = jnp.dot(piece, inner_matrix, preferred_element_type=jnp.float32).reshape(
        row_count, 2, hidden_cols
    )
    gate_part = products[:, 0, :]
    up_part = products[:, 1, :]
    hidden = (
        jax.nn.gelu(gate_part, approximate=True)
        * up_part
        * jnp.sum(membership(slots, lengths, offsets), axis=1)[:, None]
    ).astype(jnp.bfloat16)
    outer_matrix = outer_local.reshape(hidden_cols, width)
    delta = lax.psum_scatter(
        jnp.dot(hidden, outer_matrix, preferred_element_type=jnp.float32),
        "mp",
        scatter_dimension=0,
        tiled=True,
    )
    return finish(tokens_f, delta, final_gain, value_head, lengths, offsets)


MESH = pl.DeviceIdType.MESH


def mega_kernel(levels, cuts, slices, tok_ref, gain_ref, final_ref, head_ref, owner_ref, lengths_ref, offsets_ref, win_ref,
                wdown_ref, mixed_ref, rewards_ref,
                x_buf, part, swap_buf, cross_buf, first_buf, second_buf, level_buf, raw, win, wdown, hid,
                acc, mean_buf, own_mean,
                w_sem, up_send, down_send, first_send, second_send, pass_send, recv_sem,
                swap_send, swap_recv, sum_send, cross_recv, first_recv, second_recv, level_recv,
                mean_send, mean_recv):
    rep, slot = lax.axis_index("rep"), lax.axis_index("mp")
    side, row, level = slot % 2, (slot // 2) % 2, slot // 4
    parts = levels * 4
    other_rep, other_row, twin = 1 - rep, 1 - row, 1 - side
    here, cross = (rep, row), (other_rep, other_row)
    first = (rep * side + other_rep * twin, row * twin + other_row * side)
    second = (rep * twin + other_rep * side, row * side + other_row * twin)
    tok_rows, width = tok_ref.shape
    cols, count = wdown.shape[0], lengths_ref.shape[1]
    cut = width // cuts
    slab = width // slices

    def index_of(column, at):
        return at * 4 + column[0] * 2 + column[1]

    def remote(src, dst, send_sem, recv_sem, column, at, plane):
        return pltpu.make_async_remote_copy(
            src_ref=src, dst_ref=dst, send_sem=send_sem, recv_sem=recv_sem,
            device_id=(column[0], at * 4 + column[1] * 2 + plane), device_id_type=MESH,
        )

    barrier = pltpu.get_barrier_semaphore()
    pl.semaphore_signal(barrier, inc=1, device_id=(other_rep, slot), device_id_type=MESH)
    pl.semaphore_signal(barrier, inc=1, device_id=(rep, level * 4 + other_row * 2 + side), device_id_type=MESH)
    pl.semaphore_signal(barrier, inc=1, device_id=(rep, level * 4 + row * 2 + twin), device_id_type=MESH)

    @pl.loop(1, levels)
    def _(d):
        pl.semaphore_signal(barrier, inc=1, device_id=(rep, (slot + 4 * d) % parts), device_id_type=MESH)

    shares = 3
    share = width // shares

    def load_in(i):
        at = pl.ds(i * share, share)
        return pltpu.make_async_copy(win_ref.at[at], raw.at[at], w_sem.at[i])

    load_down = pltpu.make_async_copy(wdown_ref, wdown, w_sem.at[shares])
    for i in range(shares):
        load_in(i).start()
    load_down.start()

    block = 128

    def untangle(i):
        load_in(i).wait()
        to = lax.broadcasted_iota(jnp.int32, (2 * block, 2 * block), 0)
        at = lax.broadcasted_iota(jnp.int32, (2 * block, 2 * block), 1)
        pick = jnp.where((at == 2 * to) | (at == 2 * (to - block) + 1), 1.0, 0.0).astype(jnp.bfloat16)

        @pl.loop(0, share // block, unroll=2)
        def _(k):
            rows_at = pl.ds(pl.multiple_of(i * share + k * block, block), block)
            both_parts = jnp.dot(
                pick, raw[rows_at].reshape(2 * block, cols), preferred_element_type=jnp.float32
            ).astype(jnp.bfloat16)
            win[rows_at, :cols] = both_parts[:block]
            win[rows_at, cols:] = both_parts[block:]

    mine = index_of(here, level)
    tok = tok_ref[...].astype(jnp.float32)
    x_buf[mine, side] = (
        tok * lax.rsqrt(jnp.mean(tok * tok, axis=1, keepdims=True) + 1e-06) * gain_ref[...]
    ).astype(jnp.bfloat16)

    low = level < levels // 2
    inner = (level > 0) & (level < levels - 1)
    outer = jnp.logical_not(inner)

    def from_level(d):
        near = jnp.where(inner, (1, 0, 2, 3)[d], d)
        return jnp.where(low, near, levels - 1 - near)

    def piece(index, plane, s):
        return x_buf.at[index, plane, :, pl.ds(s * slab, slab)]

    def move(index, s, sem, column, at):
        return remote(piece(index, side, s), piece(index, side, s), sem.at[index, s], recv_sem.at[side, index, s],
                      column, at, side)

    def hand(index, s):
        return remote(piece(index, side, s), piece(index, side, s), pass_send.at[index, s],
                      recv_sem.at[side, index, s], here, level, twin)

    def arrive(plane, index, s):
        at = piece(index, plane, s)
        pltpu.make_async_copy(at, at, recv_sem.at[plane, index, s]).wait()

    def pass_on(index, s, upward, downward):
        @pl.when(upward & (level < levels - 1))
        def _():
            move(index, s, up_send, here, level + 1).start()

        @pl.when(downward & (level > 0))
        def _():
            move(index, s, down_send, here, level - 1).start()

        move(index, s, second_send, second, level).start()
        hand(index, s).start()

    def take(column, d, s):
        at = from_level(d)
        index = index_of(column, at)
        arrive(side, index, s)
        pass_on(index, s, at <= level, at >= level)

    def settle(column, d, s):
        index = index_of(column, from_level(d))
        arrive(side, index, s)
        hand(index, s).start()

    def collect_hands(d):
        for column in (here, first, second, cross):
            for s in range(slices):
                arrive(twin, index_of(column, from_level(d)), s)

    up_block = 256

    def up(d, n):
        lo = n * up_block
        left = x_buf[pl.ds(from_level(d) * 4, 4)].reshape(8 * tok_rows, width)
        gate = jnp.dot(left, win[:, lo:lo + up_block], preferred_element_type=jnp.float32)
        lift = jnp.dot(left, win[:, cols + lo:cols + lo + up_block], preferred_element_type=jnp.float32)
        chosen = jnp.where(owner_ref[...] == rep, 1.0, 0.0)
        hid[:, lo:lo + up_block] = (jax.nn.gelu(gate, approximate=True) * lift * chosen).astype(jnp.bfloat16)

    down_block = 512

    def down(d, q):
        at = from_level(d)

        @pl.loop(0, cut // down_block)
        def _(n):
            lo = pl.multiple_of(n * down_block, down_block)
            out = jnp.dot(hid[...], wdown[:, pl.ds(q * cut + lo, down_block)], preferred_element_type=jnp.float32)
            part[q, pl.ds(at * 4, 4), :, :, pl.ds(lo, down_block)] = out.astype(jnp.bfloat16).reshape(
                4, 2, tok_rows, down_block)

        for column in (cross, second, first, here):
            swap(index_of(column, at), q).start()

    def swap(index, q):
        return remote(part.at[q, index, twin], swap_buf.at[q, index], swap_send.at[q, index],
                      swap_recv.at[q, index], here, level, twin)

    def send(index, q, buf, sem, at, column, to):
        return remote(swap_buf.at[q, index], buf.at[q, at], sum_send.at[q, index], sem.at[q, at], column, to, side)

    def landed(buf, sem, q, at):
        pltpu.make_async_copy(buf.at[q, at], buf.at[q, at], sem.at[q, at]).wait()

    def both(index, q):
        swap(index, q).wait_recv()
        return part[q, index, side].astype(jnp.float32) + swap_buf[q, index].astype(jnp.float32)

    def reduce_outer(d, q, column, buf, sem):
        at = from_level(d)
        index = index_of(column, at)
        swap_buf[q, index] = both(index, q).astype(jnp.bfloat16)
        send(index, q, buf, sem, at, second, level).start()

    def reduce_cross(d, q):
        reduce_outer(d, q, cross, cross_buf, cross_recv)

    def reduce_second(d, q):
        reduce_outer(d, q, second, second_buf, second_recv)

    def reduce_first(d, q):
        at = from_level(d)
        index = index_of(first, at)
        total = both(index, q)
        landed(cross_buf, cross_recv, q, at)
        swap_buf[q, index] = (total + cross_buf[q, at].astype(jnp.float32)).astype(jnp.bfloat16)
        send(index, q, first_buf, first_recv, at, first, level).start()

    def reduce_here(d, q):
        at = from_level(d)
        index = index_of(here, at)
        total = both(index, q)
        landed(second_buf, second_recv, q, at)
        landed(first_buf, first_recv, q, at)
        total = total + (second_buf[q, at].astype(jnp.float32) + first_buf[q, at].astype(jnp.float32))
        if d == 0:
            acc[:, q * cut:(q + 1) * cut] = total
        else:
            swap_buf[q, index] = total.astype(jnp.bfloat16)
            send(index, q, level_buf, level_recv, level, here, at).start()

    pl.semaphore_wait(barrier, 3 + levels - 1)
    always = level >= 0
    for s in range(slices):
        move(mine, s, first_send, first, level).start()
        pass_on(mine, s, always, always)
    untangle(0)
    untangle(1)
    untangle(2)
    take(first, 0, 0)

    @pl.when(inner)
    def _():
        take(here, 1, 0)

    @pl.when(outer)
    def _():
        take(here, 1, 0)
    settle(second, 0, 0)

    @pl.when(inner)
    def _():
        take(here, 2, 0)
    settle(cross, 0, 0)
    collect_hands(0)
    up(0, 0)

    @pl.when(inner)
    def _():
        take(first, 1, 0)

    @pl.when(outer)
    def _():
        take(first, 1, 0)

    @pl.when(inner)
    def _():
        settle(second, 1, 0)

    @pl.when(outer)
    def _():
        settle(second, 1, 0)

    @pl.when(inner)
    def _():
        take(first, 2, 0)
    up(0, 1)
    up(0, 2)
    load_down.wait()
    down(0, 0)

    @pl.when(inner)
    def _():
        settle(cross, 1, 0)

    @pl.when(outer)
    def _():
        settle(cross, 1, 0)
    reduce_cross(0, 0)

    @pl.when(inner)
    def _():
        take(here, 3, 0)
    down(0, 1)
    collect_hands(1)
    reduce_second(0, 0)

    @pl.when(outer)
    def _():
        take(here, 2, 0)
        take(first, 2, 0)
    up(1, 0)

    @pl.when(inner)
    def _():
        settle(second, 2, 0)

    @pl.when(outer)
    def _():
        settle(second, 2, 0)
    reduce_cross(0, 1)
    up(1, 1)
    reduce_second(0, 1)
    up(1, 2)
    down(1, 0)

    @pl.when(outer)
    def _():
        take(here, 3, 0)
    down(1, 1)

    @pl.when(inner)
    def _():
        settle(cross, 2, 0)

    @pl.when(outer)
    def _():
        settle(cross, 2, 0)
    reduce_second(1, 0)
    reduce_second(1, 1)
    reduce_cross(1, 1)

    @pl.when(inner)
    def _():
        take(first, 3, 0)
    collect_hands(2)
    up(2, 0)
    up(2, 1)

    @pl.when(outer)
    def _():
        take(first, 3, 0)

    @pl.when(inner)
    def _():
        settle(second, 3, 0)

    @pl.when(outer)
    def _():
        settle(second, 3, 0)
    up(2, 2)
    reduce_cross(1, 0)
    down(2, 0)
    down(2, 1)
    reduce_cross(2, 0)
    reduce_second(2, 0)
    reduce_cross(2, 1)

    @pl.when(inner)
    def _():
        settle(cross, 3, 0)

    @pl.when(outer)
    def _():
        settle(cross, 3, 0)
    collect_hands(3)
    up(3, 0)
    reduce_first(2, 0)
    reduce_second(2, 1)
    up(3, 1)
    reduce_first(2, 1)
    up(3, 2)
    reduce_first(1, 1)
    reduce_first(1, 0)
    reduce_here(2, 0)
    down(3, 0)
    reduce_cross(3, 0)
    reduce_here(2, 1)
    down(3, 1)
    reduce_second(3, 0)
    reduce_cross(3, 1)
    reduce_here(1, 1)
    reduce_here(1, 0)
    reduce_second(3, 1)
    reduce_first(3, 0)
    reduce_first(3, 1)
    reduce_here(3, 0)
    reduce_first(0, 0)
    reduce_first(0, 1)
    reduce_here(3, 1)
    reduce_here(0, 1)
    reduce_here(0, 0)

    for q in range(cuts):
        @pl.loop(1, levels)
        def _(d):
            at = (level + d) % levels
            landed(level_buf, level_recv, q, at)
            acc[:, q * cut:(q + 1) * cut] += level_buf[q, at].astype(jnp.float32)

    own_slots = slot * tok_rows + lax.broadcasted_iota(jnp.int32, (tok_rows, count), 0)
    starts = offsets_ref[...]
    member = jnp.where((own_slots >= starts) & (own_slots < starts + lengths_ref[...]), 1.0, 0.0)
    live = jnp.sum(member, axis=1, keepdims=True)
    resid = tok_ref[...].astype(jnp.float32) + acc[...] * live
    scale = lax.rsqrt(jnp.mean(resid * resid, axis=1, keepdims=True) + 1e-06)
    values = jnp.sum(resid * scale * final_ref[...] * head_ref[...], axis=1, keepdims=True)
    own_mean[...] = jnp.broadcast_to(jnp.sum(values * member, axis=0, keepdims=True), own_mean.shape)

    def tell(d):
        to = (slot + d) % parts
        return pltpu.make_async_remote_copy(
            src_ref=own_mean, dst_ref=mean_buf.at[slot], send_sem=mean_send.at[to],
            recv_sem=mean_recv.at[slot], device_id=(rep, to), device_id_type=MESH,
        )

    @pl.loop(1, parts)
    def _(d):
        tell(d).start()

    mixed_ref[...] = resid.astype(jnp.bfloat16)
    acc[:8, :count] = own_mean[...]
    @pl.loop(0, slices)
    def _(s):
        move(mine, s, first_send, first, level).wait_send()

        @pl.loop(0, levels)
        def _(d):
            for column in (here, first):
                index = index_of(column, d)
                move(index, s, second_send, second, level).wait_send()

                @pl.when((d <= level) & (level < levels - 1))
                def _():
                    move(index, s, up_send, here, level).wait_send()

                @pl.when((d >= level) & (level > 0))
                def _():
                    move(index, s, down_send, here, level).wait_send()

    @pl.loop(0, parts)
    def _(i):
        for s in range(slices):
            hand(i, s).wait_send()
        for q in range(cuts):
            swap(i, q).wait_send()

    @pl.loop(0, levels)
    def _(d):
        for q in range(cuts):
            for column in (cross, second, first):
                send(index_of(column, d), q, cross_buf, cross_recv, level, second, level).wait_send()

    @pl.loop(1, levels)
    def _(d):
        for q in range(cuts):
            send(index_of(here, (level + d) % levels), q, level_buf, level_recv, level, second, level).wait_send()

    @pl.loop(1, parts)
    def _(d):
        index = (slot + parts - d) % parts
        pltpu.make_async_copy(own_mean, mean_buf.at[index], mean_recv.at[index]).wait()
        acc[:8, :count] += mean_buf[index]

    rewards_ref[...] = acc[:1, :count] / lengths_ref[...].astype(jnp.float32)

    @pl.loop(1, parts)
    def _(d):
        tell(d).wait_send()


def mega_rows(reps, parts, tokens, w_in, w_down, norm_gain, final_gain, value_head, owner, lengths, offsets):
    tok_rows, width = tokens.shape
    cols = w_in.shape[3]
    levels, cuts, slices = parts // 4, 2, 1
    cut, count = width // cuts, lengths.shape[0]
    vmem = pl.BlockSpec(memory_space=pltpu.VMEM)
    hbm = pl.BlockSpec(memory_space=pl.ANY)
    dma = pltpu.SemaphoreType.DMA
    f32, bf16 = jnp.float32, jnp.bfloat16
    few = pltpu.VMEM((cuts, levels, tok_rows, cut), bf16)
    some, each, hop = dma((cuts, levels)), dma((cuts, parts)), dma((parts, slices))
    mixed, rewards = pl.pallas_call(
        functools.partial(mega_kernel, levels, cuts, slices),
        out_shape=(
            jax.ShapeDtypeStruct((tok_rows, width), bf16),
            jax.ShapeDtypeStruct((1, count), f32),
        ),
        in_specs=[vmem] * 7 + [hbm] * 2,
        out_specs=(vmem, vmem),
        scratch_shapes=[
            pltpu.VMEM((parts, 2, tok_rows, width), bf16),
            pltpu.VMEM((cuts, parts, 2, tok_rows, cut), bf16),
            pltpu.VMEM((cuts, parts, tok_rows, cut), bf16),
            few, few, few, few,
            pltpu.VMEM((width, 2, cols), bf16),
            pltpu.VMEM((width, 2 * cols), bf16),
            pltpu.VMEM((cols, width), bf16),
            pltpu.VMEM((8 * tok_rows, cols), bf16),
            pltpu.VMEM((tok_rows, width), f32),
            pltpu.VMEM((parts, 8, count), f32),
            pltpu.VMEM((8, count), f32),
            dma((4,)), hop, hop, hop, hop, hop, dma((2, parts, slices)),
            each, each, each, some, some, some, some,
            dma((parts,)), dma((parts,)),
        ],
        compiler_params=pltpu.CompilerParams(
            collective_id=0, has_side_effects=True, vmem_limit_bytes=53477376
        ),
    )(tokens, norm_gain[None, :], final_gain[None, :], value_head[None, :], owner[None, :], lengths[None, :],
      offsets[None, :], w_in[0], w_down[0])
    return mixed, rewards[0]


def per_device(reps, parts, *args):
    tokens, w_in, w_down = args[:3]
    tok_rows, width = tokens.shape
    cols = w_in.shape[3]
    row_bytes = 2 * reps * parts * tokens.size * 2
    weight_bytes = 2 * (w_in.size + w_down.size)
    fits = tok_rows % 8 == 0 and width % 3072 == 0 and cols % 256 == 0 and args[7].shape[0] <= 128
    if reps == 2 and parts == 16 and fits and row_bytes < 2 * weight_bytes:
        return mega_rows(reps, parts, *args)
    return move_weights(*args)


def solution(mesh):
    in_specs = (
        P(("rep", "mp"), None),
        P("rep", None, None, "mp"),
        P("rep", "mp", None),
        P(),
        P(),
        P(),
        P("mp"),
        P("rep"),
        P("rep"),
    )
    out_specs = (P(("rep", "mp"), None), P("rep"))
    return jax.shard_map(
        functools.partial(per_device, mesh.shape["rep"], mesh.shape["mp"]),
        mesh=mesh, in_specs=in_specs, out_specs=out_specs, check_vma=False,
    )
```

```python
import functools

import jax
import jax.numpy as jnp
from jax import lax
from jax.experimental import pallas as pl
from jax.experimental.pallas import tpu as pltpu
from jax.sharding import PartitionSpec as P


def spread(value, axis, source):
    kept = jnp.where(lax.axis_index(axis) == source, value, 0).astype(value.dtype)
    return lax.psum(kept, axis)


def membership(slots, lengths, offsets):
    inside = (slots[:, None] >= offsets[None, :]) & (
        slots[:, None] < offsets[None, :] + lengths[None, :]
    )
    return inside.astype(jnp.float32)


def norm_rows(tokens_f, norm_gain):
    return (
        tokens_f
        * lax.rsqrt(jnp.mean(tokens_f * tokens_f, axis=1, keepdims=True) + 1e-06)
        * norm_gain
    ).astype(jnp.bfloat16)


def finish(tokens_f, delta, final_gain, value_head, lengths, offsets):
    tok_rows = tokens_f.shape[0]
    resid = tokens_f + delta
    mixed = resid.astype(jnp.bfloat16)
    final = resid * lax.rsqrt(jnp.mean(resid * resid, axis=1, keepdims=True) + 1e-06) * final_gain
    values = jnp.dot(final, value_head, precision=lax.Precision.HIGHEST)
    own_slots = lax.axis_index("mp") * tok_rows + jnp.arange(tok_rows, dtype=jnp.int32)
    member = membership(own_slots, lengths, offsets)
    partial_sums = jnp.dot(values, member, precision=lax.Precision.HIGHEST)
    totals = lax.psum(partial_sums, "mp")
    rewards = totals / lengths.astype(jnp.float32)
    return (mixed, rewards)


def move_weights(tokens, w_in, w_down, norm_gain, final_gain, value_head, owner, lengths, offsets):
    owner_index = owner[0]
    width = tokens.shape[1]
    hidden_cols = w_in.shape[3]
    tokens_f = tokens.astype(jnp.float32)
    normed = norm_rows(tokens_f, norm_gain)
    inner_local, outer_local = (
        spread(w_in, "rep", owner_index),
        spread(w_down, "rep", owner_index),
    )
    inner_matrix = inner_local.reshape(width, 2 * hidden_cols)
    piece = lax.all_gather(normed, "mp", axis=0, tiled=True)
    slots = jnp.arange(piece.shape[0], dtype=jnp.int32)
    row_count = piece.shape[0]
    products = jnp.dot(piece, inner_matrix, preferred_element_type=jnp.float32).reshape(
        row_count, 2, hidden_cols
    )
    gate_part = products[:, 0, :]
    up_part = products[:, 1, :]
    hidden = (
        jax.nn.gelu(gate_part, approximate=True)
        * up_part
        * jnp.sum(membership(slots, lengths, offsets), axis=1)[:, None]
    ).astype(jnp.bfloat16)
    outer_matrix = outer_local.reshape(hidden_cols, width)
    delta = lax.psum_scatter(
        jnp.dot(hidden, outer_matrix, preferred_element_type=jnp.float32),
        "mp",
        scatter_dimension=0,
        tiled=True,
    )
    return finish(tokens_f, delta, final_gain, value_head, lengths, offsets)


MESH = pl.DeviceIdType.MESH


def mega_kernel(levels, cuts, slices, tok_ref, gain_ref, final_ref, head_ref, owner_ref, lengths_ref, offsets_ref, win_ref,
                wdown_ref, mixed_ref, rewards_ref,
                x_buf, part, swap_buf, cross_buf, first_buf, second_buf, level_buf, near_buf, raw, win, wdown, hid,
                acc, mean_buf, own_mean,
                w_sem, up_send, down_send, first_send, second_send, pass_send, recv_sem,
                swap_send, swap_recv, sum_send, cross_recv, first_recv, second_recv, level_recv, near_recv,
                mean_send, mean_recv):
    rep, slot = lax.axis_index("rep"), lax.axis_index("mp")
    side, row, level = slot % 2, (slot // 2) % 2, slot // 4
    parts = levels * 4
    other_rep, other_row, twin = 1 - rep, 1 - row, 1 - side
    here, cross = (rep, row), (other_rep, other_row)
    first = (rep * side + other_rep * twin, row * twin + other_row * side)
    second = (rep * twin + other_rep * side, row * side + other_row * twin)
    tok_rows, width = tok_ref.shape
    cols, count = wdown.shape[0], lengths_ref.shape[1]
    cut = width // cuts
    slab = width // slices

    def index_of(column, at):
        return at * 4 + column[0] * 2 + column[1]

    def remote(src, dst, send_sem, recv_sem, column, at, plane):
        return pltpu.make_async_remote_copy(
            src_ref=src, dst_ref=dst, send_sem=send_sem, recv_sem=recv_sem,
            device_id=(column[0], at * 4 + column[1] * 2 + plane), device_id_type=MESH,
        )

    barrier = pltpu.get_barrier_semaphore()
    pl.semaphore_signal(barrier, inc=1, device_id=(other_rep, slot), device_id_type=MESH)
    pl.semaphore_signal(barrier, inc=1, device_id=(rep, level * 4 + other_row * 2 + side), device_id_type=MESH)
    pl.semaphore_signal(barrier, inc=1, device_id=(rep, level * 4 + row * 2 + twin), device_id_type=MESH)

    @pl.loop(1, levels)
    def _(d):
        pl.semaphore_signal(barrier, inc=1, device_id=(rep, (slot + 4 * d) % parts), device_id_type=MESH)

    shares = 3
    share = width // shares

    def load_in(i):
        at = pl.ds(i * share, share)
        return pltpu.make_async_copy(win_ref.at[at], raw.at[at], w_sem.at[i])

    load_down = pltpu.make_async_copy(wdown_ref, wdown, w_sem.at[shares])
    for i in range(shares):
        load_in(i).start()
    load_down.start()

    block = 128

    def untangle(i):
        load_in(i).wait()
        to = lax.broadcasted_iota(jnp.int32, (2 * block, 2 * block), 0)
        at = lax.broadcasted_iota(jnp.int32, (2 * block, 2 * block), 1)
        pick = jnp.where((at == 2 * to) | (at == 2 * (to - block) + 1), 1.0, 0.0).astype(jnp.bfloat16)

        @pl.loop(0, share // block, unroll=2)
        def _(k):
            rows_at = pl.ds(pl.multiple_of(i * share + k * block, block), block)
            both_parts = jnp.dot(
                pick, raw[rows_at].reshape(2 * block, cols), preferred_element_type=jnp.float32
            ).astype(jnp.bfloat16)
            win[rows_at, :cols] = both_parts[:block]
            win[rows_at, cols:] = both_parts[block:]

    mine = index_of(here, level)
    tok = tok_ref[...].astype(jnp.float32)
    x_buf[mine, side] = (
        tok * lax.rsqrt(jnp.mean(tok * tok, axis=1, keepdims=True) + 1e-06) * gain_ref[...]
    ).astype(jnp.bfloat16)

    low = level < levels // 2
    inner = (level > 0) & (level < levels - 1)
    outer = jnp.logical_not(inner)

    def from_level(d):
        near = jnp.where(inner, (1, 0, 2, 3)[d], d)
        return jnp.where(low, near, levels - 1 - near)

    def piece(index, plane, s):
        return x_buf.at[index, plane, :, pl.ds(s * slab, slab)]

    def move(index, s, sem, column, at):
        return remote(piece(index, side, s), piece(index, side, s), sem.at[index, s], recv_sem.at[side, index, s],
                      column, at, side)

    def hand(index, s):
        return remote(piece(index, side, s), piece(index, side, s), pass_send.at[index, s],
                      recv_sem.at[side, index, s], here, level, twin)

    def arrive(plane, index, s):
        at = piece(index, plane, s)
        pltpu.make_async_copy(at, at, recv_sem.at[plane, index, s]).wait()

    def pass_on(index, s, upward, downward):
        @pl.when(upward & (level < levels - 1))
        def _():
            move(index, s, up_send, here, level + 1).start()

        @pl.when(downward & (level > 0))
        def _():
            move(index, s, down_send, here, level - 1).start()

        move(index, s, second_send, second, level).start()
        hand(index, s).start()

    def take(column, d, s):
        at = from_level(d)
        index = index_of(column, at)
        arrive(side, index, s)
        pass_on(index, s, at <= level, at >= level)

    def settle(column, d, s):
        index = index_of(column, from_level(d))
        arrive(side, index, s)
        hand(index, s).start()

    def collect_hands(d):
        for column in (here, first, second, cross):
            for s in range(slices):
                arrive(twin, index_of(column, from_level(d)), s)

    up_block = 256

    def up(d, n):
        lo = n * up_block
        left = x_buf[pl.ds(from_level(d) * 4, 4)].reshape(8 * tok_rows, width)
        gate = jnp.dot(left, win[:, lo:lo + up_block], preferred_element_type=jnp.float32)
        lift = jnp.dot(left, win[:, cols + lo:cols + lo + up_block], preferred_element_type=jnp.float32)
        chosen = jnp.where(owner_ref[...] == rep, 1.0, 0.0)
        hid[:, lo:lo + up_block] = (jax.nn.gelu(gate, approximate=True) * lift * chosen).astype(jnp.bfloat16)

    down_block = 512

    def down(d, q):
        at = from_level(d)

        @pl.loop(0, cut // down_block)
        def _(n):
            lo = pl.multiple_of(n * down_block, down_block)
            out = jnp.dot(hid[...], wdown[:, pl.ds(q * cut + lo, down_block)], preferred_element_type=jnp.float32)
            part[q, pl.ds(at * 4, 4), :, :, pl.ds(lo, down_block)] = out.astype(jnp.bfloat16).reshape(
                4, 2, tok_rows, down_block)

        for column in (cross, second, first, here):
            swap(index_of(column, at), q).start()

    def swap(index, q):
        return remote(part.at[q, index, twin], swap_buf.at[q, index], swap_send.at[q, index],
                      swap_recv.at[q, index], here, level, twin)

    def send(index, q, buf, sem, at, column, to):
        return remote(swap_buf.at[q, index], buf.at[q, at], sum_send.at[q, index], sem.at[q, at], column, to, side)

    def landed(buf, sem, q, at):
        pltpu.make_async_copy(buf.at[q, at], buf.at[q, at], sem.at[q, at]).wait()

    def both(index, q):
        swap(index, q).wait_recv()
        return part[q, index, side].astype(jnp.float32) + swap_buf[q, index].astype(jnp.float32)

    def reduce_outer(d, q, column, buf, sem):
        at = from_level(d)
        index = index_of(column, at)
        swap_buf[q, index] = both(index, q).astype(jnp.bfloat16)
        send(index, q, buf, sem, at, second, level).start()

    def reduce_cross(d, q):
        reduce_outer(d, q, cross, cross_buf, cross_recv)

    def reduce_second(d, q):
        reduce_outer(d, q, second, second_buf, second_recv)

    def reduce_first(d, q):
        at = from_level(d)
        index = index_of(first, at)
        total = both(index, q)
        landed(cross_buf, cross_recv, q, at)
        total = total + cross_buf[q, at].astype(jnp.float32)
        if d == 0:
            beside = from_level(1)
            landed(near_buf, near_recv, q, beside)
            total = total + near_buf[q, beside].astype(jnp.float32)
        swap_buf[q, index] = total.astype(jnp.bfloat16)
        if d == 1:
            send(index, q, near_buf, near_recv, level, here, at).start()
        else:
            send(index, q, first_buf, first_recv, at, first, level).start()

    def reduce_here(d, q):
        at = from_level(d)
        index = index_of(here, at)
        total = both(index, q)
        landed(second_buf, second_recv, q, at)
        total = total + second_buf[q, at].astype(jnp.float32)
        if d != 1:
            landed(first_buf, first_recv, q, at)
            total = total + first_buf[q, at].astype(jnp.float32)
        if d == 0:
            acc[:, q * cut:(q + 1) * cut] = total
        else:
            swap_buf[q, index] = total.astype(jnp.bfloat16)
            send(index, q, level_buf, level_recv, level, here, at).start()

    pl.semaphore_wait(barrier, 3 + levels - 1)
    always = level >= 0
    for s in range(slices):
        move(mine, s, first_send, first, level).start()
        pass_on(mine, s, always, always)
    untangle(0)
    untangle(1)

    @pl.when(outer)
    def _():
        take(here, 1, 0)
    settle(second, 0, 0)
    take(first, 0, 0)

    @pl.when(inner)
    def _():
        take(here, 2, 0)
        take(here, 1, 0)
    settle(cross, 0, 0)

    @pl.when(outer)
    def _():
        take(first, 1, 0)
    untangle(2)
    collect_hands(0)
    up(0, 0)

    @pl.when(inner)
    def _():
        take(first, 1, 0)
    up(0, 1)

    @pl.when(inner)
    def _():
        take(first, 2, 0)
    up(0, 2)

    @pl.when(outer)
    def _():
        settle(second, 1, 0)
        take(here, 2, 0)
        settle(cross, 1, 0)
    load_down.wait()
    down(0, 0)
    reduce_cross(0, 0)

    @pl.when(inner)
    def _():
        settle(cross, 1, 0)
        settle(second, 1, 0)
        take(here, 3, 0)
    down(0, 1)
    collect_hands(1)

    @pl.when(outer)
    def _():
        take(first, 2, 0)
    up(1, 0)
    up(1, 1)
    up(1, 2)

    @pl.when(outer)
    def _():
        settle(second, 2, 0)

    @pl.when(inner)
    def _():
        take(first, 3, 0)
    reduce_cross(0, 1)

    @pl.when(outer)
    def _():
        settle(cross, 2, 0)

    @pl.when(inner)
    def _():
        settle(second, 2, 0)

    @pl.when(outer)
    def _():
        take(here, 3, 0)

    @pl.when(inner)
    def _():
        settle(cross, 2, 0)
    down(1, 0)
    down(1, 1)
    collect_hands(2)
    reduce_cross(1, 0)
    up(2, 0)
    reduce_cross(1, 1)
    up(2, 1)

    @pl.when(outer)
    def _():
        take(first, 3, 0)

    @pl.when(inner)
    def _():
        settle(cross, 3, 0)
    up(2, 2)
    reduce_second(1, 0)

    @pl.when(outer)
    def _():
        settle(second, 3, 0)
    down(2, 0)
    down(2, 1)
    reduce_cross(2, 0)
    reduce_first(1, 1)

    @pl.when(outer)
    def _():
        settle(cross, 3, 0)
    reduce_first(1, 0)

    @pl.when(inner)
    def _():
        settle(second, 3, 0)
    reduce_cross(2, 1)
    reduce_second(2, 0)
    reduce_second(2, 1)
    collect_hands(3)
    up(3, 0)
    reduce_here(1, 0)
    reduce_first(2, 0)
    up(3, 1)
    up(3, 2)
    reduce_first(2, 1)
    down(3, 0)
    reduce_here(2, 0)
    reduce_second(1, 1)
    reduce_cross(3, 0)
    down(3, 1)
    reduce_here(2, 1)
    reduce_cross(3, 1)
    reduce_second(3, 0)
    reduce_first(3, 0)
    reduce_first(3, 1)
    reduce_here(1, 1)
    reduce_second(3, 1)
    reduce_second(0, 0)
    reduce_first(0, 0)
    reduce_here(3, 0)
    reduce_here(3, 1)
    reduce_second(0, 1)
    reduce_first(0, 1)
    reduce_here(0, 0)
    reduce_here(0, 1)

    for q in range(cuts):
        @pl.loop(1, levels)
        def _(d):
            at = (level + d) % levels
            landed(level_buf, level_recv, q, at)
            acc[:, q * cut:(q + 1) * cut] += level_buf[q, at].astype(jnp.float32)

    own_slots = slot * tok_rows + lax.broadcasted_iota(jnp.int32, (tok_rows, count), 0)
    starts = offsets_ref[...]
    member = jnp.where((own_slots >= starts) & (own_slots < starts + lengths_ref[...]), 1.0, 0.0)
    live = jnp.sum(member, axis=1, keepdims=True)
    resid = tok_ref[...].astype(jnp.float32) + acc[...] * live
    scale = lax.rsqrt(jnp.mean(resid * resid, axis=1, keepdims=True) + 1e-06)
    values = jnp.sum(resid * scale * final_ref[...] * head_ref[...], axis=1, keepdims=True)
    own_mean[...] = jnp.broadcast_to(jnp.sum(values * member, axis=0, keepdims=True), own_mean.shape)

    def tell(d):
        to = (slot + d) % parts
        return pltpu.make_async_remote_copy(
            src_ref=own_mean, dst_ref=mean_buf.at[slot], send_sem=mean_send.at[to],
            recv_sem=mean_recv.at[slot], device_id=(rep, to), device_id_type=MESH,
        )

    @pl.loop(1, parts)
    def _(d):
        tell(d).start()

    mixed_ref[...] = resid.astype(jnp.bfloat16)
    acc[:8, :count] = own_mean[...]
    @pl.loop(0, slices)
    def _(s):
        move(mine, s, first_send, first, level).wait_send()

        @pl.loop(0, levels)
        def _(d):
            for column in (here, first):
                index = index_of(column, d)
                move(index, s, second_send, second, level).wait_send()

                @pl.when((d <= level) & (level < levels - 1))
                def _():
                    move(index, s, up_send, here, level).wait_send()

                @pl.when((d >= level) & (level > 0))
                def _():
                    move(index, s, down_send, here, level).wait_send()

    @pl.loop(0, parts)
    def _(i):
        for s in range(slices):
            hand(i, s).wait_send()
        for q in range(cuts):
            swap(i, q).wait_send()

    @pl.loop(0, levels)
    def _(d):
        for q in range(cuts):
            for column in (cross, second, first):
                send(index_of(column, d), q, cross_buf, cross_recv, level, second, level).wait_send()

    @pl.loop(1, levels)
    def _(d):
        for q in range(cuts):
            send(index_of(here, (level + d) % levels), q, level_buf, level_recv, level, second, level).wait_send()

    @pl.loop(1, parts)
    def _(d):
        index = (slot + parts - d) % parts
        pltpu.make_async_copy(own_mean, mean_buf.at[index], mean_recv.at[index]).wait()
        acc[:8, :count] += mean_buf[index]

    rewards_ref[...] = acc[:1, :count] / lengths_ref[...].astype(jnp.float32)

    @pl.loop(1, parts)
    def _(d):
        tell(d).wait_send()


def mega_rows(reps, parts, tokens, w_in, w_down, norm_gain, final_gain, value_head, owner, lengths, offsets):
    tok_rows, width = tokens.shape
    cols = w_in.shape[3]
    levels, cuts, slices = parts // 4, 2, 1
    cut, count = width // cuts, lengths.shape[0]
    vmem = pl.BlockSpec(memory_space=pltpu.VMEM)
    hbm = pl.BlockSpec(memory_space=pl.ANY)
    dma = pltpu.SemaphoreType.DMA
    f32, bf16 = jnp.float32, jnp.bfloat16
    few = pltpu.VMEM((cuts, levels, tok_rows, cut), bf16)
    some, each, hop = dma((cuts, levels)), dma((cuts, parts)), dma((parts, slices))
    mixed, rewards = pl.pallas_call(
        functools.partial(mega_kernel, levels, cuts, slices),
        out_shape=(
            jax.ShapeDtypeStruct((tok_rows, width), bf16),
            jax.ShapeDtypeStruct((1, count), f32),
        ),
        in_specs=[vmem] * 7 + [hbm] * 2,
        out_specs=(vmem, vmem),
        scratch_shapes=[
            pltpu.VMEM((parts, 2, tok_rows, width), bf16),
            pltpu.VMEM((cuts, parts, 2, tok_rows, cut), bf16),
            pltpu.VMEM((cuts, parts, tok_rows, cut), bf16),
            few, few, few, few, few,
            pltpu.VMEM((width, 2, cols), bf16),
            pltpu.VMEM((width, 2 * cols), bf16),
            pltpu.VMEM((cols, width), bf16),
            pltpu.VMEM((8 * tok_rows, cols), bf16),
            pltpu.VMEM((tok_rows, width), f32),
            pltpu.VMEM((parts, 8, count), f32),
            pltpu.VMEM((8, count), f32),
            dma((4,)), hop, hop, hop, hop, hop, dma((2, parts, slices)),
            each, each, each, some, some, some, some, some,
            dma((parts,)), dma((parts,)),
        ],
        compiler_params=pltpu.CompilerParams(
            collective_id=0, has_side_effects=True, vmem_limit_bytes=54 << 20
        ),
    )(tokens, norm_gain[None, :], final_gain[None, :], value_head[None, :], owner[None, :], lengths[None, :],
      offsets[None, :], w_in[0], w_down[0])
    return mixed, rewards[0]


def per_device(reps, parts, *args):
    tokens, w_in, w_down = args[:3]
    tok_rows, width = tokens.shape
    cols = w_in.shape[3]
    row_bytes = 2 * reps * parts * tokens.size * 2
    weight_bytes = 2 * (w_in.size + w_down.size)
    fits = tok_rows % 8 == 0 and width % 3072 == 0 and cols % 256 == 0 and args[7].shape[0] <= 128
    if reps == 2 and parts == 16 and fits and row_bytes < 2 * weight_bytes:
        return mega_rows(reps, parts, *args)
    return move_weights(*args)


def solution(mesh):
    in_specs = (
        P(("rep", "mp"), None),
        P("rep", None, None, "mp"),
        P("rep", "mp", None),
        P(),
        P(),
        P(),
        P("mp"),
        P("rep"),
        P("rep"),
    )
    out_specs = (P(("rep", "mp"), None), P("rep"))
    return jax.shard_map(
        functools.partial(per_device, mesh.shape["rep"], mesh.shape["mp"]),
        mesh=mesh, in_specs=in_specs, out_specs=out_specs, check_vma=False,
    )
```

```python
import functools

import jax
import jax.numpy as jnp
from jax import lax
from jax.experimental import pallas as pl
from jax.experimental.pallas import tpu as pltpu
from jax.sharding import PartitionSpec as P


def spread(value, axis, source):
    kept = jnp.where(lax.axis_index(axis) == source, value, 0).astype(value.dtype)
    return lax.psum(kept, axis)


def membership(slots, lengths, offsets):
    inside = (slots[:, None] >= offsets[None, :]) & (
        slots[:, None] < offsets[None, :] + lengths[None, :]
    )
    return inside.astype(jnp.float32)


def norm_rows(tokens_f, norm_gain):
    return (
        tokens_f
        * lax.rsqrt(jnp.mean(tokens_f * tokens_f, axis=1, keepdims=True) + 1e-06)
        * norm_gain
    ).astype(jnp.bfloat16)


def finish(tokens_f, delta, final_gain, value_head, lengths, offsets):
    tok_rows = tokens_f.shape[0]
    resid = tokens_f + delta
    mixed = resid.astype(jnp.bfloat16)
    final = resid * lax.rsqrt(jnp.mean(resid * resid, axis=1, keepdims=True) + 1e-06) * final_gain
    values = jnp.dot(final, value_head, precision=lax.Precision.HIGHEST)
    own_slots = lax.axis_index("mp") * tok_rows + jnp.arange(tok_rows, dtype=jnp.int32)
    member = membership(own_slots, lengths, offsets)
    partial_sums = jnp.dot(values, member, precision=lax.Precision.HIGHEST)
    totals = lax.psum(partial_sums, "mp")
    rewards = totals / lengths.astype(jnp.float32)
    return (mixed, rewards)


def move_weights(tokens, w_in, w_down, norm_gain, final_gain, value_head, owner, lengths, offsets):
    owner_index = owner[0]
    width = tokens.shape[1]
    hidden_cols = w_in.shape[3]
    tokens_f = tokens.astype(jnp.float32)
    normed = norm_rows(tokens_f, norm_gain)
    inner_local, outer_local = (
        spread(w_in, "rep", owner_index),
        spread(w_down, "rep", owner_index),
    )
    inner_matrix = inner_local.reshape(width, 2 * hidden_cols)
    piece = lax.all_gather(normed, "mp", axis=0, tiled=True)
    slots = jnp.arange(piece.shape[0], dtype=jnp.int32)
    row_count = piece.shape[0]
    products = jnp.dot(piece, inner_matrix, preferred_element_type=jnp.float32).reshape(
        row_count, 2, hidden_cols
    )
    gate_part = products[:, 0, :]
    up_part = products[:, 1, :]
    hidden = (
        jax.nn.gelu(gate_part, approximate=True)
        * up_part
        * jnp.sum(membership(slots, lengths, offsets), axis=1)[:, None]
    ).astype(jnp.bfloat16)
    outer_matrix = outer_local.reshape(hidden_cols, width)
    delta = lax.psum_scatter(
        jnp.dot(hidden, outer_matrix, preferred_element_type=jnp.float32),
        "mp",
        scatter_dimension=0,
        tiled=True,
    )
    return finish(tokens_f, delta, final_gain, value_head, lengths, offsets)


MESH = pl.DeviceIdType.MESH


def mega_kernel(levels, cuts, slices, tok_ref, gain_ref, final_ref, head_ref, owner_ref, lengths_ref, offsets_ref, win_ref,
                wdown_ref, mixed_ref, rewards_ref,
                x_buf, part, swap_buf, cross_buf, first_buf, second_buf, level_buf, near_buf, raw, win, wdown, hid,
                acc, mean_buf, own_mean,
                w_sem, up_send, down_send, first_send, second_send, pass_send, recv_sem, hand_recv,
                swap_send, swap_recv, sum_send, cross_recv, first_recv, second_recv, level_recv, near_recv,
                mean_send, mean_recv):
    rep, slot = lax.axis_index("rep"), lax.axis_index("mp")
    side, row, level = slot % 2, (slot // 2) % 2, slot // 4
    parts = levels * 4
    other_rep, other_row, twin = 1 - rep, 1 - row, 1 - side
    here, cross = (rep, row), (other_rep, other_row)
    first = (rep * side + other_rep * twin, row * twin + other_row * side)
    second = (rep * twin + other_rep * side, row * side + other_row * twin)
    tok_rows, width = tok_ref.shape
    cols, count = wdown.shape[0], lengths_ref.shape[1]
    cut = width // cuts
    slab = width // slices

    def index_of(column, at):
        return at * 4 + column[0] * 2 + column[1]

    def remote(src, dst, send_sem, recv_sem, column, at, plane):
        return pltpu.make_async_remote_copy(
            src_ref=src, dst_ref=dst, send_sem=send_sem, recv_sem=recv_sem,
            device_id=(column[0], at * 4 + column[1] * 2 + plane), device_id_type=MESH,
        )

    barrier = pltpu.get_barrier_semaphore()
    pl.semaphore_signal(barrier, inc=1, device_id=(other_rep, slot), device_id_type=MESH)
    pl.semaphore_signal(barrier, inc=1, device_id=(rep, level * 4 + other_row * 2 + side), device_id_type=MESH)
    pl.semaphore_signal(barrier, inc=1, device_id=(rep, level * 4 + row * 2 + twin), device_id_type=MESH)

    @pl.loop(1, levels)
    def _(d):
        pl.semaphore_signal(barrier, inc=1, device_id=(rep, (slot + 4 * d) % parts), device_id_type=MESH)

    shares = 3
    share = width // shares

    def load_in(i):
        at = pl.ds(i * share, share)
        return pltpu.make_async_copy(win_ref.at[at], raw.at[at], w_sem.at[i])

    load_down = pltpu.make_async_copy(wdown_ref, wdown, w_sem.at[shares])
    for i in range(shares):
        load_in(i).start()
    load_down.start()

    block = 128

    def untangle(i):
        load_in(i).wait()
        to = lax.broadcasted_iota(jnp.int32, (2 * block, 2 * block), 0)
        at = lax.broadcasted_iota(jnp.int32, (2 * block, 2 * block), 1)
        pick = jnp.where((at == 2 * to) | (at == 2 * (to - block) + 1), 1.0, 0.0).astype(jnp.bfloat16)

        @pl.loop(0, share // block, unroll=2)
        def _(k):
            rows_at = pl.ds(pl.multiple_of(i * share + k * block, block), block)
            both_parts = jnp.dot(
                pick, raw[rows_at].reshape(2 * block, cols), preferred_element_type=jnp.float32
            ).astype(jnp.bfloat16)
            win[rows_at, :cols] = both_parts[:block]
            win[rows_at, cols:] = both_parts[block:]

    mine = index_of(here, level)
    tok = tok_ref[...].astype(jnp.float32)
    x_buf[mine, side] = (
        tok * lax.rsqrt(jnp.mean(tok * tok, axis=1, keepdims=True) + 1e-06) * gain_ref[...]
    ).astype(jnp.bfloat16)

    low = level < levels // 2
    inner = (level > 0) & (level < levels - 1)
    outer = jnp.logical_not(inner)

    def from_level(d):
        near = jnp.where(inner, (1, 0, 2, 3)[d], d)
        return jnp.where(low, near, levels - 1 - near)

    def piece(index, plane, s):
        return x_buf.at[index, plane, :, pl.ds(s * slab, slab)]

    def move(index, s, sem, column, at):
        return remote(piece(index, side, s), piece(index, side, s), sem, recv_sem.at[index, s], column, at, side)

    def hand(index, s):
        return remote(piece(index, side, s), piece(index, side, s), pass_send,
                      hand_recv.at[index // 4], here, level, twin)

    def wait_for(ref, sem):
        pltpu.make_async_copy(ref, ref, sem).wait()

    def arrive(plane, index, s):
        wait_for(piece(index, plane, s), recv_sem.at[index, s])

    def pass_on(index, s, upward, downward):
        @pl.when(upward & (level < levels - 1))
        def _():
            move(index, s, up_send.at[index // 4, index % 4, s], here, level + 1).start()

        @pl.when(downward & (level > 0))
        def _():
            move(index, s, down_send.at[index // 4, index % 4, s], here, level - 1).start()

        move(index, s, second_send, second, level).start()
        hand(index, s).start()

    def take(column, d, s):
        at = from_level(d)
        index = index_of(column, at)
        arrive(side, index, s)
        pass_on(index, s, at <= level, at >= level)

    def settle(column, d, s):
        index = index_of(column, from_level(d))
        arrive(side, index, s)
        hand(index, s).start()

    def collect_hands(d):
        at = from_level(d)
        wait_for(x_buf.at[pl.ds(at * 4, 4), twin], hand_recv.at[at])

    up_block = 256

    def up(d, n):
        lo = n * up_block
        left = x_buf[pl.ds(from_level(d) * 4, 4)].reshape(8 * tok_rows, width)
        gate = jnp.dot(left, win[:, lo:lo + up_block], preferred_element_type=jnp.float32)
        lift = jnp.dot(left, win[:, cols + lo:cols + lo + up_block], preferred_element_type=jnp.float32)
        chosen = jnp.where(owner_ref[...] == rep, 1.0, 0.0)
        hid[:, lo:lo + up_block] = (jax.nn.gelu(gate, approximate=True) * lift * chosen).astype(jnp.bfloat16)

    down_block = 512

    def down(d, q):
        at = from_level(d)

        @pl.loop(0, cut // down_block)
        def _(n):
            lo = pl.multiple_of(n * down_block, down_block)
            out = jnp.dot(hid[...], wdown[:, pl.ds(q * cut + lo, down_block)], preferred_element_type=jnp.float32)
            part[q, pl.ds(at * 4, 4), :, :, pl.ds(lo, down_block)] = out.astype(jnp.bfloat16).reshape(
                4, 2, tok_rows, down_block)

        for column in (cross, second, first, here):
            swap(index_of(column, at), q).start()

    def swap(index, q):
        return remote(part.at[q, index, twin], swap_buf.at[q, index], swap_send,
                      swap_recv.at[q, index], here, level, twin)

    def send(index, q, buf, sem, at, column, to):
        return remote(swap_buf.at[q, index], buf.at[q, at], sum_send, sem.at[q, at], column, to, side)

    def landed(buf, sem, q, at):
        pltpu.make_async_copy(buf.at[q, at], buf.at[q, at], sem.at[q, at]).wait()

    def both(index, q):
        swap(index, q).wait_recv()
        return part[q, index, side].astype(jnp.float32) + swap_buf[q, index].astype(jnp.float32)

    def reduce_outer(d, q, column, buf, sem):
        at = from_level(d)
        index = index_of(column, at)
        swap_buf[q, index] = both(index, q).astype(jnp.bfloat16)
        send(index, q, buf, sem, at, second, level).start()

    def reduce_cross(d, q):
        reduce_outer(d, q, cross, cross_buf, cross_recv)

    def reduce_second(d, q):
        reduce_outer(d, q, second, second_buf, second_recv)

    def reduce_first(d, q):
        at = from_level(d)
        index = index_of(first, at)
        total = both(index, q)
        landed(cross_buf, cross_recv, q, at)
        total = total + cross_buf[q, at].astype(jnp.float32)
        if d == 0:
            beside = from_level(1)
            landed(near_buf, near_recv, q, beside)
            total = total + near_buf[q, beside].astype(jnp.float32)
        swap_buf[q, index] = total.astype(jnp.bfloat16)
        if d == 1:
            send(index, q, near_buf, near_recv, level, here, at).start()
        else:
            send(index, q, first_buf, first_recv, at, first, level).start()

    def reduce_here(d, q):
        at = from_level(d)
        index = index_of(here, at)
        total = both(index, q)
        landed(second_buf, second_recv, q, at)
        total = total + second_buf[q, at].astype(jnp.float32)
        if d != 1:
            landed(first_buf, first_recv, q, at)
            total = total + first_buf[q, at].astype(jnp.float32)
        if d == 0:
            acc[:, q * cut:(q + 1) * cut] = total
        else:
            swap_buf[q, index] = total.astype(jnp.bfloat16)
            send(index, q, level_buf, level_recv, level, here, at).start()

    pl.semaphore_wait(barrier, 3 + levels - 1)
    always = level >= 0
    for s in range(slices):
        move(mine, s, first_send, first, level).start()
        pass_on(mine, s, always, always)
    untangle(0)
    untangle(1)

    @pl.when(outer)
    def _():
        take(here, 1, 0)
    settle(second, 0, 0)
    take(first, 0, 0)

    @pl.when(inner)
    def _():
        take(here, 2, 0)
        take(here, 1, 0)
    settle(cross, 0, 0)

    @pl.when(outer)
    def _():
        take(first, 1, 0)
    untangle(2)
    collect_hands(0)
    up(0, 0)

    @pl.when(inner)
    def _():
        take(first, 1, 0)
    up(0, 1)

    @pl.when(inner)
    def _():
        take(first, 2, 0)
    up(0, 2)

    @pl.when(outer)
    def _():
        settle(second, 1, 0)
        take(here, 2, 0)
        settle(cross, 1, 0)
    load_down.wait()
    down(0, 0)
    reduce_cross(0, 0)

    @pl.when(inner)
    def _():
        settle(cross, 1, 0)
        settle(second, 1, 0)
        take(here, 3, 0)
    down(0, 1)
    collect_hands(1)

    @pl.when(outer)
    def _():
        take(first, 2, 0)
    up(1, 0)
    up(1, 1)
    up(1, 2)

    @pl.when(outer)
    def _():
        settle(second, 2, 0)

    @pl.when(inner)
    def _():
        take(first, 3, 0)
    reduce_cross(0, 1)

    @pl.when(outer)
    def _():
        settle(cross, 2, 0)

    @pl.when(inner)
    def _():
        settle(second, 2, 0)

    @pl.when(outer)
    def _():
        take(here, 3, 0)

    @pl.when(inner)
    def _():
        settle(cross, 2, 0)
    down(1, 0)
    down(1, 1)
    collect_hands(2)
    reduce_cross(1, 0)
    up(2, 0)
    reduce_cross(1, 1)
    up(2, 1)

    @pl.when(outer)
    def _():
        take(first, 3, 0)

    @pl.when(inner)
    def _():
        settle(cross, 3, 0)
    up(2, 2)
    reduce_second(1, 0)

    @pl.when(outer)
    def _():
        settle(second, 3, 0)
    down(2, 0)
    down(2, 1)
    reduce_cross(2, 0)
    reduce_first(1, 1)

    @pl.when(outer)
    def _():
        settle(cross, 3, 0)
    reduce_first(1, 0)

    @pl.when(inner)
    def _():
        settle(second, 3, 0)
    reduce_cross(2, 1)
    reduce_second(2, 0)
    reduce_second(2, 1)
    collect_hands(3)
    up(3, 0)
    reduce_here(1, 0)
    reduce_first(2, 0)
    up(3, 1)
    up(3, 2)
    reduce_first(2, 1)
    down(3, 0)
    reduce_here(2, 0)
    reduce_second(1, 1)
    reduce_cross(3, 0)
    down(3, 1)
    reduce_here(2, 1)
    reduce_cross(3, 1)
    reduce_second(3, 0)
    reduce_first(3, 0)
    reduce_first(3, 1)
    reduce_here(1, 1)
    reduce_second(3, 1)
    reduce_second(0, 0)
    reduce_first(0, 0)
    reduce_here(3, 0)
    reduce_here(3, 1)
    reduce_second(0, 1)
    reduce_first(0, 1)
    reduce_here(0, 0)
    reduce_here(0, 1)

    for q in range(cuts):
        @pl.loop(1, levels)
        def _(d):
            at = (level + d) % levels
            landed(level_buf, level_recv, q, at)
            acc[:, q * cut:(q + 1) * cut] += level_buf[q, at].astype(jnp.float32)

    own_slots = slot * tok_rows + lax.broadcasted_iota(jnp.int32, (tok_rows, count), 0)
    starts = offsets_ref[...]
    member = jnp.where((own_slots >= starts) & (own_slots < starts + lengths_ref[...]), 1.0, 0.0)
    live = jnp.sum(member, axis=1, keepdims=True)
    resid = tok_ref[...].astype(jnp.float32) + acc[...] * live
    scale = lax.rsqrt(jnp.mean(resid * resid, axis=1, keepdims=True) + 1e-06)
    values = jnp.sum(resid * scale * final_ref[...] * head_ref[...], axis=1, keepdims=True)
    own_mean[...] = jnp.broadcast_to(jnp.sum(values * member, axis=0, keepdims=True), own_mean.shape)

    def tell(d):
        to = (slot + d) % parts
        return pltpu.make_async_remote_copy(
            src_ref=own_mean, dst_ref=mean_buf.at[slot], send_sem=mean_send,
            recv_sem=mean_recv, device_id=(rep, to), device_id_type=MESH,
        )

    @pl.loop(1, parts)
    def _(d):
        tell(d).start()

    mixed_ref[...] = resid.astype(jnp.bfloat16)
    acc[:8, :count] = own_mean[...]
    @pl.loop(0, levels)
    def _(d):
        for s in range(slices):
            for column in (here, first):
                index = index_of(column, d)

                @pl.when((d <= level) & (level < levels - 1))
                def _():
                    move(index, s, up_send.at[index // 4, index % 4, s], here, level).wait_send()

                @pl.when((d >= level) & (level > 0))
                def _():
                    move(index, s, down_send.at[index // 4, index % 4, s], here, level).wait_send()

    wait_for(x_buf.at[mine, side], first_send)
    wait_for(x_buf.at[pl.ds(0, levels)], second_send)
    wait_for(x_buf.at[pl.ds(0, parts // 2)], pass_send)
    wait_for(swap_buf, swap_send)
    wait_for(swap_buf.at[:, pl.ds(0, parts - 1)], sum_send)
    wait_for(mean_buf.at[pl.ds(0, parts - 1)], mean_recv)

    @pl.loop(1, parts)
    def _(d):
        acc[:8, :count] += mean_buf[(slot + parts - d) % parts]

    rewards_ref[...] = acc[:1, :count] / lengths_ref[...].astype(jnp.float32)

    wait_for(mean_buf.at[pl.ds(0, parts - 1)], mean_send)


def mega_rows(reps, parts, tokens, w_in, w_down, norm_gain, final_gain, value_head, owner, lengths, offsets):
    tok_rows, width = tokens.shape
    cols = w_in.shape[3]
    levels, cuts, slices = parts // 4, 2, 1
    cut, count = width // cuts, lengths.shape[0]
    vmem = pl.BlockSpec(memory_space=pltpu.VMEM)
    hbm = pl.BlockSpec(memory_space=pl.ANY)
    dma = pltpu.SemaphoreType.DMA
    f32, bf16 = jnp.float32, jnp.bfloat16
    few = pltpu.VMEM((cuts, levels, tok_rows, cut), bf16)
    some, each, hop = dma((cuts, levels)), dma((cuts, parts)), dma((parts, slices))
    mixed, rewards = pl.pallas_call(
        functools.partial(mega_kernel, levels, cuts, slices),
        out_shape=(
            jax.ShapeDtypeStruct((tok_rows, width), bf16),
            jax.ShapeDtypeStruct((1, count), f32),
        ),
        in_specs=[vmem] * 7 + [hbm] * 2,
        out_specs=(vmem, vmem),
        scratch_shapes=[
            pltpu.VMEM((parts, 2, tok_rows, width), bf16),
            pltpu.VMEM((cuts, parts, 2, tok_rows, cut), bf16),
            pltpu.VMEM((cuts, parts, tok_rows, cut), bf16),
            few, few, few, few, few,
            pltpu.VMEM((width, 2, cols), bf16),
            pltpu.VMEM((width, 2 * cols), bf16),
            pltpu.VMEM((cols, width), bf16),
            pltpu.VMEM((8 * tok_rows, cols), bf16),
            pltpu.VMEM((tok_rows, width), f32),
            pltpu.VMEM((parts, 8, count), f32),
            pltpu.VMEM((8, count), f32),
            dma((4,)), dma((levels, 4, slices)), dma((levels, 4, slices)), dma, dma, dma, hop, dma((levels,)),
            dma, each, dma, some, some, some, some, some,
            dma, dma,
        ],
        compiler_params=pltpu.CompilerParams(
            collective_id=0, has_side_effects=True, vmem_limit_bytes=54 << 20
        ),
    )(tokens, norm_gain[None, :], final_gain[None, :], value_head[None, :], owner[None, :], lengths[None, :],
      offsets[None, :], w_in[0], w_down[0])
    return mixed, rewards[0]


def per_device(reps, parts, *args):
    tokens, w_in, w_down = args[:3]
    tok_rows, width = tokens.shape
    cols = w_in.shape[3]
    row_bytes = 2 * reps * parts * tokens.size * 2
    weight_bytes = 2 * (w_in.size + w_down.size)
    fits = tok_rows % 8 == 0 and width % 3072 == 0 and cols % 256 == 0 and args[7].shape[0] <= 128
    if reps == 2 and parts == 16 and fits and row_bytes < 2 * weight_bytes:
        return mega_rows(reps, parts, *args)
    return move_weights(*args)


def solution(mesh):
    in_specs = (
        P(("rep", "mp"), None),
        P("rep", None, None, "mp"),
        P("rep", "mp", None),
        P(),
        P(),
        P(),
        P("mp"),
        P("rep"),
        P("rep"),
    )
    out_specs = (P(("rep", "mp"), None), P("rep"))
    return jax.shard_map(
        functools.partial(per_device, mesh.shape["rep"], mesh.shape["mp"]),
        mesh=mesh, in_specs=in_specs, out_specs=out_specs, check_vma=False,
    )
```

```python
import functools

import jax
import jax.numpy as jnp
from jax import lax
from jax.experimental import pallas as pl
from jax.experimental.pallas import tpu as pltpu
from jax.sharding import PartitionSpec as P


def spread(value, axis, source):
    kept = jnp.where(lax.axis_index(axis) == source, value, 0).astype(value.dtype)
    return lax.psum(kept, axis)


def membership(slots, lengths, offsets):
    inside = (slots[:, None] >= offsets[None, :]) & (
        slots[:, None] < offsets[None, :] + lengths[None, :]
    )
    return inside.astype(jnp.float32)


def norm_rows(tokens_f, norm_gain):
    return (
        tokens_f
        * lax.rsqrt(jnp.mean(tokens_f * tokens_f, axis=1, keepdims=True) + 1e-06)
        * norm_gain
    ).astype(jnp.bfloat16)


def finish(tokens_f, delta, final_gain, value_head, lengths, offsets):
    tok_rows = tokens_f.shape[0]
    resid = tokens_f + delta
    mixed = resid.astype(jnp.bfloat16)
    final = resid * lax.rsqrt(jnp.mean(resid * resid, axis=1, keepdims=True) + 1e-06) * final_gain
    values = jnp.dot(final, value_head, precision=lax.Precision.HIGHEST)
    own_slots = lax.axis_index("mp") * tok_rows + jnp.arange(tok_rows, dtype=jnp.int32)
    member = membership(own_slots, lengths, offsets)
    partial_sums = jnp.dot(values, member, precision=lax.Precision.HIGHEST)
    totals = lax.psum(partial_sums, "mp")
    rewards = totals / lengths.astype(jnp.float32)
    return (mixed, rewards)


def move_weights(tokens, w_in, w_down, norm_gain, final_gain, value_head, owner, lengths, offsets):
    owner_index = owner[0]
    width = tokens.shape[1]
    hidden_cols = w_in.shape[3]
    tokens_f = tokens.astype(jnp.float32)
    normed = norm_rows(tokens_f, norm_gain)
    inner_local, outer_local = (
        spread(w_in, "rep", owner_index),
        spread(w_down, "rep", owner_index),
    )
    inner_matrix = inner_local.reshape(width, 2 * hidden_cols)
    piece = lax.all_gather(normed, "mp", axis=0, tiled=True)
    slots = jnp.arange(piece.shape[0], dtype=jnp.int32)
    row_count = piece.shape[0]
    products = jnp.dot(piece, inner_matrix, preferred_element_type=jnp.float32).reshape(
        row_count, 2, hidden_cols
    )
    gate_part = products[:, 0, :]
    up_part = products[:, 1, :]
    hidden = (
        jax.nn.gelu(gate_part, approximate=True)
        * up_part
        * jnp.sum(membership(slots, lengths, offsets), axis=1)[:, None]
    ).astype(jnp.bfloat16)
    outer_matrix = outer_local.reshape(hidden_cols, width)
    delta = lax.psum_scatter(
        jnp.dot(hidden, outer_matrix, preferred_element_type=jnp.float32),
        "mp",
        scatter_dimension=0,
        tiled=True,
    )
    return finish(tokens_f, delta, final_gain, value_head, lengths, offsets)


MESH = pl.DeviceIdType.MESH


def mega_kernel(levels, cuts, slices, tok_ref, gain_ref, final_ref, head_ref, owner_ref, lengths_ref, offsets_ref, win_ref,
                wdown_ref, mixed_ref, rewards_ref,
                x_buf, part, swap_buf, cross_buf, first_buf, second_buf, level_buf, near_buf, raw, win, wdown, hid,
                acc, mean_buf, own_mean,
                w_sem, up_send, down_send, first_send, second_send, pass_send, recv_sem, hand_recv,
                swap_send, swap_recv, sum_send, cross_recv, first_recv, second_recv, level_recv, near_recv,
                mean_send, mean_recv):
    rep, slot = lax.axis_index("rep"), lax.axis_index("mp")
    side, row, level = slot % 2, (slot // 2) % 2, slot // 4
    parts = levels * 4
    other_rep, other_row, twin = 1 - rep, 1 - row, 1 - side
    here, cross = (rep, row), (other_rep, other_row)
    first = (rep * side + other_rep * twin, row * twin + other_row * side)
    second = (rep * twin + other_rep * side, row * side + other_row * twin)
    tok_rows, width = tok_ref.shape
    cols, count = wdown.shape[0], lengths_ref.shape[1]
    cut = width // cuts
    slab = width // slices

    def index_of(column, at):
        return at * 4 + column[0] * 2 + column[1]

    def remote(src, dst, send_sem, recv_sem, column, at, plane):
        return pltpu.make_async_remote_copy(
            src_ref=src, dst_ref=dst, send_sem=send_sem, recv_sem=recv_sem,
            device_id=(column[0], at * 4 + column[1] * 2 + plane), device_id_type=MESH,
        )

    barrier = pltpu.get_barrier_semaphore()
    pl.semaphore_signal(barrier, inc=1, device_id=(other_rep, slot), device_id_type=MESH)
    pl.semaphore_signal(barrier, inc=1, device_id=(rep, level * 4 + other_row * 2 + side), device_id_type=MESH)
    pl.semaphore_signal(barrier, inc=1, device_id=(rep, level * 4 + row * 2 + twin), device_id_type=MESH)

    @pl.loop(1, levels)
    def _(d):
        pl.semaphore_signal(barrier, inc=1, device_id=(rep, (slot + 4 * d) % parts), device_id_type=MESH)

    shares = 3
    share = width // shares

    def load_in(i):
        at = pl.ds(i * share, share)
        return pltpu.make_async_copy(win_ref.at[at], raw.at[at], w_sem.at[i])

    load_down = pltpu.make_async_copy(wdown_ref, wdown, w_sem.at[shares])
    for i in range(shares):
        load_in(i).start()
    load_down.start()

    block = 128

    def untangle(i):
        load_in(i).wait()
        to = lax.broadcasted_iota(jnp.int32, (2 * block, 2 * block), 0)
        at = lax.broadcasted_iota(jnp.int32, (2 * block, 2 * block), 1)
        pick = jnp.where((at == 2 * to) | (at == 2 * (to - block) + 1), 1.0, 0.0).astype(jnp.bfloat16)

        @pl.loop(0, share // block, unroll=2)
        def _(k):
            rows_at = pl.ds(pl.multiple_of(i * share + k * block, block), block)
            both_parts = jnp.dot(
                pick, raw[rows_at].reshape(2 * block, cols), preferred_element_type=jnp.float32
            ).astype(jnp.bfloat16)
            win[rows_at, :cols] = both_parts[:block]
            win[rows_at, cols:] = both_parts[block:]

    mine = index_of(here, level)
    tok = tok_ref[...].astype(jnp.float32)
    x_buf[mine, side] = (
        tok * lax.rsqrt(jnp.mean(tok * tok, axis=1, keepdims=True) + 1e-06) * gain_ref[...]
    ).astype(jnp.bfloat16)

    low = level < levels // 2
    inner = (level > 0) & (level < levels - 1)
    outer = jnp.logical_not(inner)

    def from_level(d):
        near = jnp.where(inner, (1, 0, 2, 3)[d], d)
        return jnp.where(low, near, levels - 1 - near)

    def piece(index, plane, s):
        return x_buf.at[index, plane, :, pl.ds(s * slab, slab)]

    def move(index, s, sem, column, at):
        return remote(piece(index, side, s), piece(index, side, s), sem, recv_sem.at[index, s], column, at, side)

    def hand(index, s):
        return remote(piece(index, side, s), piece(index, side, s), pass_send,
                      hand_recv.at[index // 4], here, level, twin)

    def wait_for(ref, sem):
        pltpu.make_async_copy(ref, ref, sem).wait()

    def arrive(plane, index, s):
        wait_for(piece(index, plane, s), recv_sem.at[index, s])

    def pass_on(index, s, upward, downward):
        @pl.when(upward & (level < levels - 1))
        def _():
            move(index, s, up_send.at[index // 4, index % 4, s], here, level + 1).start()

        @pl.when(downward & (level > 0))
        def _():
            move(index, s, down_send.at[index // 4, index % 4, s], here, level - 1).start()

        move(index, s, second_send, second, level).start()
        hand(index, s).start()

    def take(column, d, s):
        at = from_level(d)
        index = index_of(column, at)
        arrive(side, index, s)
        pass_on(index, s, at <= level, at >= level)

    def settle(column, d, s):
        index = index_of(column, from_level(d))
        arrive(side, index, s)
        hand(index, s).start()

    def collect_hands(d):
        at = from_level(d)
        wait_for(x_buf.at[pl.ds(at * 4, 4), twin], hand_recv.at[at])

    up_block = 256

    def up(d, n):
        lo = n * up_block
        left = x_buf[pl.ds(from_level(d) * 4, 4)].reshape(8 * tok_rows, width)
        gate = jnp.dot(left, win[:, lo:lo + up_block], preferred_element_type=jnp.float32)
        lift = jnp.dot(left, win[:, cols + lo:cols + lo + up_block], preferred_element_type=jnp.float32)
        chosen = jnp.where(owner_ref[...] == rep, 1.0, 0.0)
        hid[:, lo:lo + up_block] = (jax.nn.gelu(gate, approximate=True) * lift * chosen).astype(jnp.bfloat16)

    down_block = 512

    def down(d, q):
        at = from_level(d)

        @pl.loop(0, cut // down_block)
        def _(n):
            lo = pl.multiple_of(n * down_block, down_block)
            out = jnp.dot(hid[...], wdown[:, pl.ds(q * cut + lo, down_block)], preferred_element_type=jnp.float32)
            part[q, pl.ds(at * 4, 4), :, :, pl.ds(lo, down_block)] = out.astype(jnp.bfloat16).reshape(
                4, 2, tok_rows, down_block)

        for column in (cross, second, first, here):
            swap(index_of(column, at), q).start()

    def swap(index, q):
        return remote(part.at[q, index, twin], swap_buf.at[q, index], swap_send,
                      swap_recv.at[q, index // 4], here, level, twin)

    def send(index, q, buf, sem, at, column, to):
        return remote(swap_buf.at[q, index], buf.at[q, at], sum_send, sem.at[q, at], column, to, side)

    def landed(buf, sem, q, at):
        pltpu.make_async_copy(buf.at[q, at], buf.at[q, at], sem.at[q, at]).wait()

    def both(index, q):
        return part[q, index, side].astype(jnp.float32) + swap_buf[q, index].astype(jnp.float32)

    def reduce_outer(d, q, column, buf, sem):
        at = from_level(d)
        index = index_of(column, at)
        swap_buf[q, index] = both(index, q).astype(jnp.bfloat16)
        send(index, q, buf, sem, at, second, level).start()

    def reduce_cross(d, q):
        at = from_level(d)
        wait_for(swap_buf.at[q, pl.ds(at * 4, 4)], swap_recv.at[q, at])
        reduce_outer(d, q, cross, cross_buf, cross_recv)

    def reduce_second(d, q):
        reduce_outer(d, q, second, second_buf, second_recv)

    def reduce_first(d, q):
        at = from_level(d)
        index = index_of(first, at)
        total = both(index, q)
        landed(cross_buf, cross_recv, q, at)
        total = total + cross_buf[q, at].astype(jnp.float32)
        if d == 0:
            beside = from_level(1)
            landed(near_buf, near_recv, q, beside)
            total = total + near_buf[q, beside].astype(jnp.float32)
        swap_buf[q, index] = total.astype(jnp.bfloat16)
        if d == 1:
            send(index, q, near_buf, near_recv, level, here, at).start()
        else:
            send(index, q, first_buf, first_recv, at, first, level).start()

    def reduce_here(d, q):
        at = from_level(d)
        index = index_of(here, at)
        total = both(index, q)
        landed(second_buf, second_recv, q, at)
        total = total + second_buf[q, at].astype(jnp.float32)
        if d != 1:
            landed(first_buf, first_recv, q, at)
            total = total + first_buf[q, at].astype(jnp.float32)
        if d == 0:
            acc[:, q * cut:(q + 1) * cut] = total
        else:
            swap_buf[q, index] = total.astype(jnp.bfloat16)
            send(index, q, level_buf, level_recv, level, here, at).start()

    pl.semaphore_wait(barrier, 3 + levels - 1)
    always = level >= 0
    for s in range(slices):
        move(mine, s, first_send, first, level).start()
        pass_on(mine, s, always, always)
    untangle(0)
    untangle(1)

    @pl.when(outer)
    def _():
        take(here, 1, 0)
    settle(second, 0, 0)
    take(first, 0, 0)

    @pl.when(inner)
    def _():
        take(here, 2, 0)
        take(here, 1, 0)
    settle(cross, 0, 0)

    @pl.when(outer)
    def _():
        take(first, 1, 0)
    untangle(2)
    collect_hands(0)
    up(0, 0)

    @pl.when(inner)
    def _():
        take(first, 1, 0)
    up(0, 1)

    @pl.when(inner)
    def _():
        take(first, 2, 0)
    up(0, 2)

    @pl.when(outer)
    def _():
        settle(second, 1, 0)
        take(here, 2, 0)
        settle(cross, 1, 0)
    load_down.wait()
    down(0, 0)
    reduce_cross(0, 0)

    @pl.when(inner)
    def _():
        settle(cross, 1, 0)
        settle(second, 1, 0)
        take(here, 3, 0)
    down(0, 1)
    collect_hands(1)

    @pl.when(outer)
    def _():
        take(first, 2, 0)
    up(1, 0)
    up(1, 1)
    up(1, 2)

    @pl.when(outer)
    def _():
        settle(second, 2, 0)

    @pl.when(inner)
    def _():
        take(first, 3, 0)
    reduce_cross(0, 1)

    @pl.when(outer)
    def _():
        settle(cross, 2, 0)

    @pl.when(inner)
    def _():
        settle(second, 2, 0)

    @pl.when(outer)
    def _():
        take(here, 3, 0)

    @pl.when(inner)
    def _():
        settle(cross, 2, 0)
    down(1, 0)
    down(1, 1)
    collect_hands(2)
    reduce_cross(1, 0)
    up(2, 0)
    reduce_cross(1, 1)
    up(2, 1)

    @pl.when(outer)
    def _():
        take(first, 3, 0)

    @pl.when(inner)
    def _():
        settle(cross, 3, 0)
    up(2, 2)
    reduce_second(1, 0)

    @pl.when(outer)
    def _():
        settle(second, 3, 0)
    down(2, 0)
    down(2, 1)
    reduce_cross(2, 0)
    reduce_first(1, 1)

    @pl.when(outer)
    def _():
        settle(cross, 3, 0)
    reduce_first(1, 0)

    @pl.when(inner)
    def _():
        settle(second, 3, 0)
    reduce_cross(2, 1)
    reduce_second(2, 0)
    reduce_second(2, 1)
    collect_hands(3)
    up(3, 0)
    reduce_here(1, 0)
    reduce_first(2, 0)
    up(3, 1)
    up(3, 2)
    reduce_first(2, 1)
    down(3, 0)
    reduce_here(2, 0)
    reduce_second(1, 1)
    reduce_cross(3, 0)
    down(3, 1)
    reduce_here(2, 1)
    reduce_cross(3, 1)
    reduce_second(3, 0)
    reduce_first(3, 0)
    reduce_first(3, 1)
    reduce_here(1, 1)
    reduce_second(3, 1)
    reduce_second(0, 0)
    reduce_first(0, 0)
    reduce_here(3, 0)
    reduce_here(3, 1)
    reduce_second(0, 1)
    reduce_first(0, 1)
    reduce_here(0, 0)
    reduce_here(0, 1)

    for q in range(cuts):
        @pl.loop(1, levels)
        def _(d):
            at = (level + d) % levels
            landed(level_buf, level_recv, q, at)
            acc[:, q * cut:(q + 1) * cut] += level_buf[q, at].astype(jnp.float32)

    own_slots = slot * tok_rows + lax.broadcasted_iota(jnp.int32, (tok_rows, count), 0)
    starts = offsets_ref[...]
    member = jnp.where((own_slots >= starts) & (own_slots < starts + lengths_ref[...]), 1.0, 0.0)
    live = jnp.sum(member, axis=1, keepdims=True)
    resid = tok_ref[...].astype(jnp.float32) + acc[...] * live
    scale = lax.rsqrt(jnp.mean(resid * resid, axis=1, keepdims=True) + 1e-06)
    values = jnp.sum(resid * scale * final_ref[...] * head_ref[...], axis=1, keepdims=True)
    own_mean[...] = jnp.broadcast_to(jnp.sum(values * member, axis=0, keepdims=True), own_mean.shape)

    def tell(d):
        to = (slot + d) % parts
        return pltpu.make_async_remote_copy(
            src_ref=own_mean, dst_ref=mean_buf.at[slot], send_sem=mean_send,
            recv_sem=mean_recv, device_id=(rep, to), device_id_type=MESH,
        )

    @pl.loop(1, parts)
    def _(d):
        tell(d).start()

    mixed_ref[...] = resid.astype(jnp.bfloat16)
    acc[:8, :count] = own_mean[...]
    @pl.loop(0, levels)
    def _(d):
        for s in range(slices):
            for column in (here, first):
                index = index_of(column, d)

                @pl.when((d <= level) & (level < levels - 1))
                def _():
                    move(index, s, up_send.at[index // 4, index % 4, s], here, level).wait_send()

                @pl.when((d >= level) & (level > 0))
                def _():
                    move(index, s, down_send.at[index // 4, index % 4, s], here, level).wait_send()

    wait_for(x_buf.at[mine, side], first_send)
    wait_for(x_buf.at[pl.ds(0, levels)], second_send)
    wait_for(x_buf.at[pl.ds(0, parts // 2)], pass_send)
    wait_for(swap_buf, swap_send)
    wait_for(swap_buf.at[:, pl.ds(0, parts - 1)], sum_send)
    wait_for(mean_buf.at[pl.ds(0, parts - 1)], mean_recv)

    @pl.loop(1, parts)
    def _(d):
        acc[:8, :count] += mean_buf[(slot + parts - d) % parts]

    rewards_ref[...] = acc[:1, :count] / lengths_ref[...].astype(jnp.float32)

    wait_for(mean_buf.at[pl.ds(0, parts - 1)], mean_send)


def mega_rows(reps, parts, tokens, w_in, w_down, norm_gain, final_gain, value_head, owner, lengths, offsets):
    tok_rows, width = tokens.shape
    cols = w_in.shape[3]
    levels, cuts, slices = parts // 4, 2, 1
    cut, count = width // cuts, lengths.shape[0]
    vmem = pl.BlockSpec(memory_space=pltpu.VMEM)
    hbm = pl.BlockSpec(memory_space=pl.ANY)
    dma = pltpu.SemaphoreType.DMA
    f32, bf16 = jnp.float32, jnp.bfloat16
    few = pltpu.VMEM((cuts, levels, tok_rows, cut), bf16)
    some, each, hop = dma((cuts, levels)), dma((cuts, parts)), dma((parts, slices))
    mixed, rewards = pl.pallas_call(
        functools.partial(mega_kernel, levels, cuts, slices),
        out_shape=(
            jax.ShapeDtypeStruct((tok_rows, width), bf16),
            jax.ShapeDtypeStruct((1, count), f32),
        ),
        in_specs=[vmem] * 7 + [hbm] * 2,
        out_specs=(vmem, vmem),
        scratch_shapes=[
            pltpu.VMEM((parts, 2, tok_rows, width), bf16),
            pltpu.VMEM((cuts, parts, 2, tok_rows, cut), bf16),
            pltpu.VMEM((cuts, parts, tok_rows, cut), bf16),
            few, few, few, few, few,
            pltpu.VMEM((width, 2, cols), bf16),
            pltpu.VMEM((width, 2 * cols), bf16),
            pltpu.VMEM((cols, width), bf16),
            pltpu.VMEM((8 * tok_rows, cols), bf16),
            pltpu.VMEM((tok_rows, width), f32),
            pltpu.VMEM((parts, 8, count), f32),
            pltpu.VMEM((8, count), f32),
            dma((4,)), dma((levels, 4, slices)), dma((levels, 4, slices)), dma, dma, dma, hop, dma((levels,)),
            dma, some, dma, some, some, some, some, some,
            dma, dma,
        ],
        compiler_params=pltpu.CompilerParams(
            collective_id=0, has_side_effects=True, vmem_limit_bytes=54 << 20
        ),
    )(tokens, norm_gain[None, :], final_gain[None, :], value_head[None, :], owner[None, :], lengths[None, :],
      offsets[None, :], w_in[0], w_down[0])
    return mixed, rewards[0]


def per_device(reps, parts, *args):
    tokens, w_in, w_down = args[:3]
    tok_rows, width = tokens.shape
    cols = w_in.shape[3]
    row_bytes = 2 * reps * parts * tokens.size * 2
    weight_bytes = 2 * (w_in.size + w_down.size)
    fits = tok_rows % 8 == 0 and width % 3072 == 0 and cols % 256 == 0 and args[7].shape[0] <= 128
    if reps == 2 and parts == 16 and fits and row_bytes < 2 * weight_bytes:
        return mega_rows(reps, parts, *args)
    return move_weights(*args)


def solution(mesh):
    in_specs = (
        P(("rep", "mp"), None),
        P("rep", None, None, "mp"),
        P("rep", "mp", None),
        P(),
        P(),
        P(),
        P("mp"),
        P("rep"),
        P("rep"),
    )
    out_specs = (P(("rep", "mp"), None), P("rep"))
    return jax.shard_map(
        functools.partial(per_device, mesh.shape["rep"], mesh.shape["mp"]),
        mesh=mesh, in_specs=in_specs, out_specs=out_specs, check_vma=False,
    )
```
